256 devices in a mesh: seq: 64 (over z, x, y_hi), head: 4 (over y_lo, core).
Axes of the slice: x: 4, y: 4 (y_hi: 2, y_lo: 2; y = y_hi * 2 + y_lo), z: 8, core: 2. Of those that a mesh axis runs over, the one named last changes fastest.
Arguments:
- queries: bfloat16 [16384, 4096], P('seq', 'head'), may hold values from -48 to 48
- key_rows: bfloat16 [16384, 4096], P('seq', 'head'), may hold values from -4 to 4
- value_rows: bfloat16 [16384, 4096], P('seq', 'head'), may hold values from -6 to 6
- out_grad: bfloat16 [16384, 2048], P('seq', 'head'), may hold values from -6 to 6
- out_proj: bfloat16 [4096, 2048], P('head'), may hold values from -0.125 to 0.125
- section_table: int32 [32, 3], P('head'), may hold values 0 or 1
- block_active: int32 [64, 3], P('seq'), may hold values 0 or 1
Outputs:
- query_grad: bfloat16 [16384, 4096], P('seq', 'head')
- key_grad: bfloat16 [16384, 4096], P('seq', 'head')
- value_grad: bfloat16 [16384, 4096], P('seq', 'head')
The draws below stay inside these ranges and needn't reach their ends.
All inputs are finite; a program needn't handle non-finite values.
Results may differ from the reference program's by a relative error of at most 0.008.
Values may be sent and summed in bfloat16 or wider, within the bound.
A program may use at most 64 MiB of HBM per device.

```python
import math
from functools import partial
from functools import reduce
import jax
import jax.numpy as jnp
from jax import lax

BLK = 256
HEADS = 32
HDIM = 128
DMODEL = 2048
SECTIONS = 3
NBLOCKS = 64
TOKENS = 16384


def paired_fields(key):
    base_key = jax.random.fold_in(key, 4021)
    field_shape = (TOKENS, HEADS * HDIM)
    key_field = jnp.clip(jax.random.normal(jax.random.fold_in(base_key, 1), field_shape, jnp.float32), -4.0, 4.0)
    query_field = jnp.clip(jax.random.normal(jax.random.fold_in(base_key, 2), field_shape, jnp.float32), -4.0, 4.0)
    return (query_field, key_field)


def draw_queries(key, part):
    return paired_fields(key)[0].astype(jnp.bfloat16)


def draw_key_rows(key, part):
    return paired_fields(key)[1].astype(jnp.bfloat16)


def plant(values, key, smallest, top_value):
    shape = values.shape
    spot = [jax.random.randint(jax.random.fold_in(key, axis), (), 0, shape[axis]) for axis in range(len(shape))]
    values = values.at[tuple(spot)].set(smallest)
    longest = shape.index(max(shape))
    spot[longest] = (spot[longest] + 1) % shape[longest]
    return values.at[tuple(spot)].set(top_value)


def steps_of(rng, shape, shards, smallest, largest):
    factor_of, own = 1.0, jax.random.fold_in(rng, 6)
    for dim, shards_of in shards:
        heights = jnp.exp(jax.random.uniform(jax.random.fold_in(own, dim), (shards_of,), jnp.float32, smallest / len(shards), largest / len(shards)))
        factor_of = factor_of * jnp.repeat(heights, shape[dim] // shards_of).reshape([-1 if axis == dim else 1 for axis in range(len(shape))])
    return factor_of


def centred(own_key, dims, width, bound, split=(), held_as=jnp.bfloat16):
    drawn = width * jax.random.normal(own_key, dims, jnp.float32)
    if split:
        drawn = drawn * steps_of(own_key, dims, split, -0.22, 0.18)
    return jnp.clip(drawn, -bound, bound).astype(held_as)


def setup_inputs(seed: int = 0) -> dict:
    key_list = jax.random.split(jax.random.key(seed), 8)
    return {
        "queries": draw_queries(jax.random.fold_in(key_list[7], 71), 0),
        "key_rows": draw_key_rows(jax.random.fold_in(key_list[7], 71), 0),
        "value_rows": centred(key_list[2], (TOKENS, HEADS * HDIM), 1.0, 6.0, ((0, 64), (1, 4))),
        "out_grad": centred(key_list[3], (TOKENS, DMODEL), 1.0, 6.0, ((0, 64), (1, 4))),
        "out_proj": centred(key_list[4], (HEADS * HDIM, DMODEL), DMODEL ** -0.5, 0.125, ((0, 4),)),
        "section_table": plant((jax.random.randint(key_list[5], (HEADS, SECTIONS), 0, 3) < 2).astype(jnp.int32), jax.random.fold_in(key_list[5], 1), 0, 1),
        "block_active": plant((jax.random.randint(key_list[6], (NBLOCKS, SECTIONS), 0, 4) < 3).astype(jnp.int32), jax.random.fold_in(key_list[6], 1), 0, 1),
    }


def shift_down(blocks, count):
    filler = jnp.zeros((count,) + blocks.shape[1:], blocks.dtype)
    return jnp.concatenate([filler, blocks[:blocks.shape[0] - count]], axis=0)

def shift_up(blocks, count):
    filler = jnp.zeros((count,) + blocks.shape[1:], blocks.dtype)
    return jnp.concatenate([blocks[count:], filler], axis=0)

def to_wide(array):
    return array.astype(jnp.float32)

def narrow(array):
    return lax.optimization_barrier(array.astype(jnp.bfloat16)).astype(jnp.float32)

def head_grads(block_active, operands):
    query_h, key_h, value_h, grad_h, head_flags = operands
    score_scale = 1.0 / math.sqrt(HDIM)
    query_wide = to_wide(query_h)
    key_wide = to_wide(key_h)
    value_wide = to_wide(value_h)
    grad_wide = to_wide(grad_h)
    row_ids = jnp.arange(BLK)
    causal = (row_ids[:, None] >= row_ids[None, :])[None]
    block_ids = jnp.arange(NBLOCKS)
    key_sets = [(key_wide, value_wide, causal, 0)]
    for section_index in range(SECTIONS):
        shift_count = NBLOCKS // 2 ** (section_index + 1)
        usable = (head_flags[section_index] * block_active[:, section_index] > 0) & (block_ids >= shift_count)
        key_sets.append((shift_down(key_wide, shift_count), shift_down(value_wide, shift_count), usable[:, None, None], shift_count))
    logits = []
    for key_entry in key_sets:
        raw_scores = jnp.einsum('bid,bjd->bij', query_wide, key_entry[0]) * score_scale
        logits.append(jnp.where(key_entry[2], raw_scores, -1e+30))
    row_max = reduce(jnp.maximum, [lax.optimization_barrier(jnp.max(logit_set, axis=-1)) for logit_set in logits])
    row_sum = reduce(jnp.add, [lax.optimization_barrier(jnp.sum(jnp.exp(logit_set - row_max[..., None]), axis=-1)) for logit_set in logits])
    log_norm = row_max + jnp.log(row_sum)
    probs_list = [jnp.where(key_entry[2], jnp.exp(logit_set - log_norm[..., None]), 0.0) for logit_set, key_entry in zip(logits, key_sets)]
    weight_list = [narrow(prob_set) for prob_set in probs_list]
    context = reduce(jnp.add, [jnp.einsum('bij,bjd->bid', weight_set, key_entry[1]) for weight_set, key_entry in zip(weight_list, key_sets)])
    row_delta = lax.optimization_barrier(jnp.sum(grad_wide * context, axis=-1))
    query_grad = jnp.zeros_like(query_wide)
    key_grad = jnp.zeros_like(query_wide)
    value_grad = jnp.zeros_like(query_wide)
    for set_index in range(SECTIONS + 1):
        key_part, value_part, allowed, shift_count = key_sets[set_index]
        prob_grad = jnp.einsum('bid,bjd->bij', grad_wide, value_part)
        dlogit = narrow(probs_list[set_index] * (prob_grad - row_delta[..., None]) * score_scale)
        query_grad = query_grad + jnp.einsum('bij,bjd->bid', dlogit, key_part)
        key_term = jnp.einsum('bij,bid->bjd', dlogit, query_wide)
        value_term = jnp.einsum('bij,bid->bjd', weight_list[set_index], grad_wide)
        if set_index > 0:
            key_term = narrow(key_term)
            value_term = narrow(value_term)
        key_grad = key_grad + shift_up(key_term, shift_count)
        value_grad = value_grad + shift_up(value_term, shift_count)
    return (query_grad.astype(jnp.bfloat16), key_grad.astype(jnp.bfloat16), value_grad.astype(jnp.bfloat16))

def by_heads(matrix):
    return matrix.reshape(NBLOCKS, BLK, HEADS, HDIM).transpose(2, 0, 1, 3)

def from_heads(stacked):
    return stacked.transpose(1, 2, 0, 3).reshape(TOKENS, HEADS * HDIM)

def reference(queries, key_rows, value_rows, out_grad, out_proj, section_table, block_active):
    attn_grad = jnp.dot(out_grad, out_proj.T, preferred_element_type=jnp.float32).astype(jnp.bfloat16)
    operands = (by_heads(queries), by_heads(key_rows), by_heads(value_rows), by_heads(attn_grad), section_table)
    query_out, key_out, value_out = lax.map(partial(head_grads, block_active), operands)
    return (from_heads(query_out), from_heads(key_out), from_heads(value_out))
```

```python
import functools
import math

import jax
import jax.numpy as jnp
from jax import lax
from jax.experimental import pallas as pl
from jax.experimental.pallas import tpu as pltpu
from jax.sharding import PartitionSpec as P

BLK = 256
HDIM = 128
SECTIONS = 3
LAG = 2
AHEAD = 3
MESH = pl.DeviceIdType.MESH
HIDE = -1e30
SCALE = 1.0 / math.sqrt(HDIM)
NT = (((1,), (1,)), ((), ()))
TN = (((0,), (0,)), ((), ()))
NN = (((1,), (0,)), ((), ()))


def mm(a, b, dims):
    return lax.dot_general(a, b, dims, preferred_element_type=jnp.float32)


def kernel(
    seq_count, head_count, bias, q_in, k_in, v_in, og_in, w_in, dq, dk, dv,
    qa, ga, ka, va, og, w, scores, slopes, own_dk, own_dv, sent, got,
    local_sem, og_send, og_recv, bulk_send, bulk_recv, row_send, row_recv,
):
    heads = q_in.shape[1] // HDIM
    seq = lax.axis_index("seq")
    me = lax.axis_index("head")
    stride = seq_count // 8

    def along(steps):
        return {"seq": lax.rem(seq + (steps % 8) * stride, seq_count)}

    def peer(offset):
        return {"head": lax.rem(me + offset, head_count)}

    def cols(h):
        return pl.ds(pl.multiple_of(h * HDIM, HDIM), HDIM)

    bulk = {"k": (ka, 0, 1), "v": (va, 1, 1), "q": (qa, 2, -1), "g": (ga, 3, -1)}

    def move(kind, hop, h):
        ref, row, sign = bulk[kind]
        return pltpu.make_async_remote_copy(
            src_ref=ref.at[hop, :, cols(h)],
            dst_ref=ref.at[hop + 1, :, cols(h)],
            send_sem=bulk_send.at[row, hop, h],
            recv_sem=bulk_recv.at[row, hop, h],
            device_id=along(sign * (2 if hop == 2 else 1)),
            device_id_type=MESH,
        )

    def rows_move(hop, h):
        return pltpu.make_async_remote_copy(
            src_ref=sent.at[hop, h],
            dst_ref=got.at[hop, h],
            send_sem=row_send.at[hop, h],
            recv_sem=row_recv.at[hop, h],
            device_id=along(-(1, 2, 4)[hop]),
            device_id_type=MESH,
        )

    def og_move(offset):
        return pltpu.make_async_remote_copy(
            src_ref=og.at[0],
            dst_ref=og.at[head_count - offset],
            send_sem=og_send.at[offset - 1],
            recv_sem=og_recv.at[head_count - offset - 1],
            device_id=peer(offset),
            device_id_type=MESH,
        )

    locals_ = [
        pltpu.make_async_copy(source, target, local_sem.at[index])
        for index, (source, target) in enumerate(
            ((k_in, ka.at[0]), (v_in, va.at[0]), (q_in, qa.at[0]), (og_in, og.at[0]), (w_in, w))
        )
    ]
    for copy in locals_:
        copy.start()

    barrier = pltpu.get_barrier_semaphore()
    for steps in (1, -1, 2, -2, 4):
        pl.semaphore_signal(barrier, inc=1, device_id=along(steps), device_id_type=MESH)
    for offset in range(1, head_count):
        pl.semaphore_signal(barrier, inc=1, device_id=peer(offset), device_id_type=MESH)
    pl.semaphore_wait(barrier, 5 + head_count - 1)

    for copy in locals_[:4]:
        copy.wait()
    for offset in range(1, head_count):
        og_move(offset).start()

    @pl.loop(0, heads)
    def _(h):
        for kind in "kvq":
            move(kind, 0, h).start()

    locals_[4].wait()
    for offset in range(1, head_count):
        og_move(head_count - offset).wait_recv()
    width = og.shape[2]

    @pl.loop(0, heads // 2)
    def _(pair):
        wide = pl.ds(pl.multiple_of(pair * 2 * HDIM, 2 * HDIM), 2 * HDIM)
        total = jnp.zeros((BLK, 2 * HDIM), jnp.float32)
        for offset in range(head_count):
            owner = lax.rem(me + offset, head_count)
            features = pl.ds(pl.multiple_of(owner * width, width), width)
            total = total + mm(og[offset], w[wide, features], NT)
        ga[0, :, wide] = total.astype(jnp.bfloat16)

    @pl.loop(0, heads)
    def _(h):
        move("g", 0, h).start()

    @pl.loop(0, heads)
    def _(h):
        for kind in "kvq":
            move(kind, 0, h).wait_recv()
            move(kind, 1, h).start()

    @pl.loop(0, heads)
    def _(h):
        move("g", 0, h).wait_recv()
        move("g", 1, h).start()

    @pl.loop(0, heads)
    def _(h):
        for kind in "kv":
            move(kind, 1, h).wait_recv()
            move(kind, 2, h).start()
        for kind in "qg":
            move(kind, 1, h).wait_recv()

        @pl.when(h < AHEAD)
        def _():
            for kind in "qg":
                move(kind, 2, h).start()

    def query_side(h):
        at = cols(h)
        query = qa[0, :, at]
        grad = ga[0, :, at]
        key_index = lax.broadcasted_iota(jnp.int32, (BLK, BLK), 0)
        query_index = lax.broadcasted_iota(jnp.int32, (BLK, BLK), 1)
        top = None
        for s in range(SECTIONS + 1):
            raw = mm(ka[s, :, at], query, NT) * SCALE
            if s == 0:
                raw = jnp.where(key_index <= query_index, raw, HIDE)
            else:
                raw = raw + bias[(SECTIONS - s) * heads + h]
            scores[s] = raw
            high = jnp.max(raw, axis=0, keepdims=True)
            top = high if top is None else jnp.maximum(top, high)
        total = None
        for s in range(SECTIONS + 1):
            part = jnp.exp(scores[s] - top)
            scores[s] = part
            part = jnp.sum(part, axis=0, keepdims=True)
            total = part if total is None else total + part
        inverse = 1.0 / total
        delta = None
        for s in range(SECTIONS + 1):
            probs = scores[s] * inverse
            scores[s] = probs
            weights = probs.astype(jnp.bfloat16)
            slope = mm(va[s, :, at], grad, NT)
            slopes[s] = slope
            part = jnp.sum(weights.astype(jnp.float32) * slope, axis=0, keepdims=True)
            delta = part if delta is None else delta + part
            if s == 0:
                own_dv[:, at] = mm(weights, grad, NN)
        log_norm = top + jnp.log(total)
        for hop in range(SECTIONS):
            sent[hop, h, 0:1, :] = log_norm - bias[(SECTIONS - 1 - hop) * heads + h]
            sent[hop, h, 1:2, :] = delta
        query_sum = None
        for s in range(SECTIONS + 1):
            dlogit = (scores[s] * (slopes[s] - delta) * SCALE).astype(jnp.bfloat16)
            part = mm(dlogit, ka[s, :, at], TN)
            query_sum = part if query_sum is None else query_sum + part
            if s == 0:
                own_dk[:, at] = mm(dlogit, query, NN)
        dq[:, at] = query_sum.astype(jnp.bfloat16)

    def key_side(h):
        at = cols(h)
        key = ka[0, :, at]
        value = va[0, :, at]
        key_sum = own_dk[:, at]
        value_sum = own_dv[:, at]
        for hop in range(SECTIONS):
            query = qa[hop + 1, :, at]
            grad = ga[hop + 1, :, at]
            log_norm = got[hop, h, 0:1, :]
            delta = got[hop, h, 1:2, :]
            probs = jnp.exp(mm(key, query, NT) * SCALE - log_norm)
            slope = mm(value, grad, NT)
            dlogit = (probs * (slope - delta) * SCALE).astype(jnp.bfloat16)
            key_sum = key_sum + mm(dlogit, query, NN)
            value_sum = value_sum + mm(probs.astype(jnp.bfloat16), grad, NN)
        dk[:, at] = key_sum.astype(jnp.bfloat16)
        dv[:, at] = value_sum.astype(jnp.bfloat16)

    @pl.loop(0, heads + LAG)
    def _(step):
        @pl.when(step + AHEAD < heads)
        def _():
            for kind in "qg":
                move(kind, 2, step + AHEAD).start()

        @pl.when(step < heads)
        def _():
            for kind in "kv":
                move(kind, 2, step).wait_recv()
            query_side(step)
            for hop in range(SECTIONS):
                rows_move(hop, step).start()

        @pl.when(step >= LAG)
        def _():
            h = step - LAG
            for kind in "qg":
                move(kind, 2, h).wait_recv()
            for hop in range(SECTIONS):
                rows_move(hop, h).wait_recv()
            key_side(h)

    @pl.loop(0, heads)
    def _(h):
        for hop in range(SECTIONS):
            rows_move(hop, h).wait_send()
            for kind in "kvqg":
                move(kind, hop, h).wait_send()

    for offset in range(1, head_count):
        og_move(offset).wait_send()


def body(queries, key_rows, value_rows, out_grad, out_proj, section_table, block_active):
    seq_count = lax.axis_size("seq")
    head_count = lax.axis_size("head")
    heads = queries.shape[1] // HDIM
    position = lax.axis_index("seq")
    spans = jnp.array([seq_count // 2 ** (index + 1) for index in range(SECTIONS)], jnp.int32)
    usable = (section_table.T * block_active[0][:, None] > 0) & (position >= spans)[:, None]
    bias = jnp.where(usable, 0.0, HIDE).astype(jnp.float32).reshape(SECTIONS * heads)
    width = queries.shape[1]
    four = (SECTIONS + 1, BLK, width)
    any_space = pl.BlockSpec(memory_space=pl.ANY)
    vmem = pl.BlockSpec(memory_space=pltpu.VMEM)
    out = jax.ShapeDtypeStruct((BLK, width), jnp.bfloat16)
    return pl.pallas_call(
        functools.partial(kernel, seq_count, head_count),
        out_shape=(out, out, out),
        in_specs=[pl.BlockSpec(memory_space=pltpu.SMEM)] + [any_space] * 5,
        out_specs=(vmem, vmem, vmem),
        scratch_shapes=[
            pltpu.VMEM(four, jnp.bfloat16),
            pltpu.VMEM(four, jnp.bfloat16),
            pltpu.VMEM(four, jnp.bfloat16),
            pltpu.VMEM(four, jnp.bfloat16),
            pltpu.VMEM((head_count, *out_grad.shape), jnp.bfloat16),
            pltpu.VMEM(out_proj.shape, jnp.bfloat16),
            pltpu.VMEM((SECTIONS + 1, BLK, BLK), jnp.float32),
            pltpu.VMEM((SECTIONS + 1, BLK, BLK), jnp.float32),
            pltpu.VMEM((BLK, width), jnp.float32),
            pltpu.VMEM((BLK, width), jnp.float32),
            pltpu.VMEM((SECTIONS, heads, 2, BLK), jnp.float32),
            pltpu.VMEM((SECTIONS, heads, 2, BLK), jnp.float32),
            pltpu.SemaphoreType.DMA((5,)),
            pltpu.SemaphoreType.DMA((head_count - 1,)),
            pltpu.SemaphoreType.DMA((head_count - 1,)),
            pltpu.SemaphoreType.DMA((4, SECTIONS, heads)),
            pltpu.SemaphoreType.DMA((4, SECTIONS, heads)),
            pltpu.SemaphoreType.DMA((SECTIONS, heads)),
            pltpu.SemaphoreType.DMA((SECTIONS, heads)),
        ],
        compiler_params=pltpu.CompilerParams(
            collective_id=0, has_side_effects=True, vmem_limit_bytes=60 * 1024 * 1024
        ),
        name="attention_grads",
    )(bias, queries, key_rows, value_rows, out_grad, out_proj)


def solution(mesh):
    return jax.shard_map(
        body,
        mesh=mesh,
        in_specs=(
            P("seq", "head"),
            P("seq", "head"),
            P("seq", "head"),
            P("seq", "head"),
            P("head", None),
            P("head", None),
            P("seq", None),
        ),
        out_specs=(P("seq", "head"), P("seq", "head"), P("seq", "head")),
        check_vma=False,
    )
```

```python
import functools
import math

import jax
import jax.numpy as jnp
from jax import lax
from jax.experimental import pallas as pl
from jax.experimental.pallas import tpu as pltpu
from jax.sharding import PartitionSpec as P

BLK = 256
HDIM = 128
SECTIONS = 3
MESH = pl.DeviceIdType.MESH
HIDE = -1e30
SCALE = 1.0 / math.sqrt(HDIM)
NT = (((1,), (1,)), ((), ()))
TN = (((0,), (0,)), ((), ()))
NN = (((1,), (0,)), ((), ()))


def mm(a, b, dims):
    return lax.dot_general(a, b, dims, preferred_element_type=jnp.float32)


def kernel(
    seq_count, moved, table, active, q_in, k_in, v_in, og_in, w_in, dq, dk, dv,
    qa, ga, ka, va, og, w, scores, slopes, held_p, held_s, tops, norms, own_dk, own_dv, parts,
    stat_out, stat_in, row_out, row_in, back_out, back_in,
    local_sem, og_send, og_recv, near_send, near_recv, bulk_send, bulk_recv,
    stat_send, stat_recv, row_send, row_recv, back_send, back_recv,
):
    heads = q_in.shape[1] // HDIM
    width = og_in.shape[1]
    seq = lax.axis_index("seq")
    me = lax.axis_index("head")
    stride = seq_count // 8
    mates = (me, me + 1 - 2 * (me % 2), me + 2 - 4 * (me // 2), 3 - me)

    def along(steps):
        return {"seq": lax.rem(seq + (steps % 8) * stride, seq_count)}

    def cols(h):
        return pl.ds(pl.multiple_of(h * HDIM, HDIM), HDIM)

    def remote(source, target, send, recv, device):
        return pltpu.make_async_remote_copy(
            src_ref=source, dst_ref=target, send_sem=send, recv_sem=recv,
            device_id=device, device_id_type=MESH,
        )

    bulk = {"k": (ka, 0, 1), "v": (va, 1, 1), "q": (qa, 2, -1)}

    def move(kind, hop, h):
        ref, row, sign = bulk[kind]
        return remote(
            ref.at[hop, :, cols(h)], ref.at[hop + 1, :, cols(h)],
            bulk_send.at[row, hop, h], bulk_recv.at[row, hop, h],
            along(sign * (2 if hop == 2 else 1)),
        )

    def og_move(hop):
        return remote(
            og.at[hop, 0], og.at[hop + 1, 0], og_send.at[hop], og_recv.at[hop],
            along(-(2 if hop == 2 else 1)),
        )

    def near(slot, which):
        source, target, mate = ((0, 1, 1), (0, 2, 2), (2, 3, 1))[which]
        return remote(
            og.at[slot, source], og.at[slot, target], near_send.at[slot, which],
            near_recv.at[slot, which], {"head": mates[mate]},
        )

    def stat_move(hop, h):
        return remote(
            stat_out.at[hop, h], stat_in.at[hop, h], stat_send.at[hop, h], stat_recv.at[hop, h],
            along((1, 2, 4)[hop]),
        )

    def row_move(hop, h):
        return remote(
            row_out.at[hop, h], row_in.at[hop, h], row_send.at[hop, h], row_recv.at[hop, h],
            along(-(1, 2, 4)[hop]),
        )

    def back_move(hop, h):
        return remote(
            back_out.at[hop, :, cols(h)], back_in.at[hop, :, cols(h)],
            back_send.at[hop, h], back_recv.at[hop, h], along((2, 1, 1)[hop]),
        )

    def hidden(hop, h):
        index = SECTIONS - 1 - hop
        inside = (seq >= seq_count // 2 ** (index + 1)).astype(jnp.int32)
        usable = table[index, h] * active[0, index] * inside
        return (1.0 - usable.astype(jnp.float32)) * HIDE

    def causal(raw):
        key_index = lax.broadcasted_iota(jnp.int32, (BLK, BLK), 0)
        query_index = lax.broadcasted_iota(jnp.int32, (BLK, BLK), 1)
        return jnp.where(key_index <= query_index, raw, HIDE)

    def make_grad(slot):
        near(slot, 0).wait_recv()
        near(slot, 2).wait_recv()

        @pl.loop(0, heads // 2)
        def _(pair):
            wide = pl.ds(pl.multiple_of(pair * 2 * HDIM, 2 * HDIM), 2 * HDIM)
            total = jnp.zeros((BLK, 2 * HDIM), jnp.float32)
            for index, owner in enumerate(mates):
                features = pl.ds(pl.multiple_of(owner * width, width), width)
                total = total + mm(og[slot, index], w[wide, features], NT)
            ga[slot, :, wide] = total.astype(jnp.bfloat16)

    def pass_near(slot):
        near(slot, 1).wait_recv()
        near(slot, 2).start()

    def query_side(h):
        at = cols(h)
        query = qa[0, :, at]
        grad = ga[0, :, at]
        top = None
        for s in range(SECTIONS + 1):
            raw = mm(ka[s, :, at], query, NT) * SCALE
            raw = causal(raw) if s == 0 else raw + hidden(s - 1, h)
            scores[s] = raw
            high = jnp.max(raw, axis=0, keepdims=True)
            top = high if top is None else jnp.maximum(top, high)
        total = None
        for s in range(SECTIONS + 1):
            part = jnp.exp(scores[s] - top)
            scores[s] = part
            part = jnp.sum(part, axis=0, keepdims=True)
            total = part if total is None else total + part
        inverse = 1.0 / total
        delta = None
        for s in range(SECTIONS + 1):
            probs = scores[s] * inverse
            scores[s] = probs
            weights = probs.astype(jnp.bfloat16)
            slope = mm(va[s, :, at], grad, NT)
            slopes[s] = slope
            part = jnp.sum(weights.astype(jnp.float32) * slope, axis=0, keepdims=True)
            delta = part if delta is None else delta + part
            if s == 0:
                own_dv[:, at] = mm(weights, grad, NN)
        log_norm = top + jnp.log(total)
        for hop in range(SECTIONS):
            row_out[hop, h, 0:1, :] = log_norm - hidden(hop, h)
            row_out[hop, h, 1:2, :] = delta
        query_sum = None
        for s in range(SECTIONS + 1):
            dlogit = (scores[s] * (slopes[s] - delta) * SCALE).astype(jnp.bfloat16)
            part = mm(dlogit, ka[s, :, at], TN)
            query_sum = part if query_sum is None else query_sum + part
            if s == 0:
                own_dk[:, at] = mm(dlogit, query, NN)
        dq[:, at] = query_sum.astype(jnp.bfloat16)
        for hop in range(SECTIONS):
            row_move(hop, h).start()

    def key_side(h):
        at = cols(h)
        key = ka[0, :, at]
        value = va[0, :, at]
        key_sum = own_dk[:, at]
        value_sum = own_dv[:, at]
        for hop in range(SECTIONS):
            query = qa[hop + 1, :, at]
            grad = ga[hop + 1, :, at]
            log_norm = row_in[hop, h, 0:1, :]
            delta = row_in[hop, h, 1:2, :]
            probs = jnp.exp(mm(key, query, NT) * SCALE - log_norm)
            slope = mm(value, grad, NT)
            dlogit = (probs * (slope - delta) * SCALE).astype(jnp.bfloat16)
            key_sum = key_sum + mm(dlogit, query, NN)
            value_sum = value_sum + mm(probs.astype(jnp.bfloat16), grad, NN)
        dk[:, at] = key_sum.astype(jnp.bfloat16)
        dv[:, at] = value_sum.astype(jnp.bfloat16)

    def partial_scores(slot, h):
        at = cols(h)
        raw = mm(ka[0, :, at], qa[slot, :, at], NT) * SCALE
        if slot == 0:
            raw = causal(raw)
        top = jnp.max(raw, axis=0, keepdims=True)
        part = jnp.exp(raw - top)
        slope = mm(va[0, :, at], ga[slot, :, at], NT)
        held_p[slot, h] = part
        held_s[slot, h] = slope
        total = jnp.sum(part, axis=0, keepdims=True)
        drift = jnp.sum(part * slope, axis=0, keepdims=True)
        tops[slot, h, 0:1, :] = top
        return top, total, drift

    def stage_own(h):
        top, total, drift = partial_scores(0, h)
        norms[h, 0:1, :] = total
        norms[h, 1:2, :] = drift

    def stage_a(h):
        for kind in ("q",):
            move(kind, 2, h).wait_recv()
        for hop in range(SECTIONS):
            top, total, drift = partial_scores(hop + 1, h)
            stat_out[hop, h, 0:1, :] = top
            stat_out[hop, h, 1:2, :] = total
            stat_out[hop, h, 2:3, :] = drift
            stat_out[hop, h, 3:4, :] = drift
            stat_move(hop, h).start()

    def stage_b(h):
        for hop in range(SECTIONS):
            stat_move(hop, h).wait_recv()
        tops_of = [tops[0, h, 0:1, :]] + [
            stat_in[hop, h, 0:1, :] + hidden(hop, h) for hop in range(SECTIONS)
        ]
        top = functools.reduce(jnp.maximum, tops_of)
        factor = jnp.exp(tops_of[0] - top)
        total = factor * norms[h, 0:1, :]
        drift = factor * norms[h, 1:2, :]
        for hop in range(SECTIONS):
            factor = jnp.exp(tops_of[hop + 1] - top)
            total = total + factor * stat_in[hop, h, 1:2, :]
            drift = drift + factor * stat_in[hop, h, 2:3, :]
        log_norm = top + jnp.log(total)
        delta = drift / total
        norms[h, 0:1, :] = log_norm
        norms[h, 1:2, :] = delta
        for hop in range(SECTIONS):
            row_out[hop, h, 0:1, :] = log_norm - hidden(hop, h)
            row_out[hop, h, 1:2, :] = delta
            row_move(hop, h).start()

    def stage_c(h):
        at = cols(h)
        for hop in range(SECTIONS):
            row_move(hop, h).wait_recv()
        key_sum = None
        value_sum = None
        for slot in (3, 2, 1, 0):
            if slot == 0:
                log_norm, delta = norms[h, 0:1, :], norms[h, 1:2, :]
            else:
                log_norm, delta = row_in[slot - 1, h, 0:1, :], row_in[slot - 1, h, 1:2, :]
            probs = held_p[slot, h] * jnp.exp(tops[slot, h, 0:1, :] - log_norm)
            dlogit = (probs * (held_s[slot, h] - delta) * SCALE).astype(jnp.bfloat16)
            query_part = mm(dlogit, ka[0, :, at], TN)
            if slot == 3:
                back_out[0, :, at] = query_part.astype(jnp.bfloat16)
            else:
                parts[slot, :, at] = query_part
            key_part = mm(dlogit, qa[slot, :, at], NN)
            value_part = mm(probs.astype(jnp.bfloat16), ga[slot, :, at], NN)
            key_sum = key_part if key_sum is None else key_sum + key_part
            value_sum = value_part if value_sum is None else value_sum + value_part
        dk[:, at] = key_sum.astype(jnp.bfloat16)
        dv[:, at] = value_sum.astype(jnp.bfloat16)
        back_move(0, h).start()

    def stage_back(hop, h):
        at = cols(h)
        back_move(hop, h).wait_recv()
        total = (parts[2 - hop, :, at] + back_in[hop, :, at].astype(jnp.float32)).astype(jnp.bfloat16)
        if hop == 2:
            dq[:, at] = total
        else:
            back_out[hop + 1, :, at] = total
            back_move(hop + 1, h).start()

    copies = [
        pltpu.make_async_copy(source, target, local_sem.at[index])
        for index, (source, target) in enumerate(
            ((og_in, og.at[0, 0]), (q_in, qa.at[0]), (k_in, ka.at[0]), (v_in, va.at[0]), (w_in, w))
        )
    ]
    for copy in copies:
        copy.start()

    barrier = pltpu.get_barrier_semaphore()
    for steps in (1, -1, 2, -2, 4):
        pl.semaphore_signal(barrier, inc=1, device_id=along(steps), device_id_type=MESH)
    for mate in mates[1:3]:
        pl.semaphore_signal(barrier, inc=1, device_id={"head": mate}, device_id_type=MESH)
    pl.semaphore_wait(barrier, 7)

    def each(first, last):
        return pl.loop(first, last)

    copies[0].wait()
    og_move(0).start()
    near(0, 1).start()
    near(0, 0).start()
    copies[1].wait()

    @each(0, 2)
    def _(h):
        move("q", 0, h).start()

    copies[2].wait()
    copies[3].wait()

    @each(moved, heads)
    def _(h):
        move("k", 0, h).start()
        move("v", 0, h).start()

    og_move(0).wait_recv()
    og_move(1).start()
    near(1, 1).start()
    near(1, 0).start()

    @each(2, 4)
    def _(h):
        move("q", 0, h).start()

    pass_near(0)

    @each(0, 2)
    def _(h):
        move("q", 0, h).wait_recv()
        move("q", 1, h).start()

    @each(moved, heads)
    def _(h):
        for kind in "kv":
            move(kind, 0, h).wait_recv()
            move(kind, 1, h).start()

    og_move(1).wait_recv()
    og_move(2).start()
    near(2, 1).start()
    near(2, 0).start()

    @each(4, heads)
    def _(h):
        move("q", 0, h).start()

    pass_near(1)

    @each(2, heads)
    def _(h):
        move("q", 0, h).wait_recv()
        move("q", 1, h).start()

    copies[4].wait()
    make_grad(0)

    @each(moved, heads)
    def _(h):
        for kind in "kv":
            move(kind, 1, h).wait_recv()
            move(kind, 2, h).start()

    @each(0, 4)
    def _(h):
        move("q", 1, h).wait_recv()
        move("q", 2, h).start()

    pass_near(2)
    og_move(2).wait_recv()
    near(3, 1).start()
    near(3, 0).start()

    make_grad(1)
    make_grad(2)

    @each(4, heads)
    def _(h):
        move("q", 1, h).wait_recv()

    @each(0, moved)
    def _(h):
        stage_own(h)

    pass_near(3)

    @each(moved, heads - 2)
    def _(h):
        for kind in "kv":
            move(kind, 2, h).wait_recv()
        query_side(h)

    make_grad(3)

    @each(heads - 2, heads)
    def _(h):
        for kind in "kv":
            move(kind, 2, h).wait_recv()
        query_side(h)

    lag_b, lag_c, lag_d, lag_e, lag_f = 2, 3, 5, 7, 9
    lead = 3

    @each(0, moved + lag_f)
    def _(step):
        def when(low, high, action):
            @pl.when((step >= low) & (step < high))
            def _():
                action(step - low)

        when(1, 1 + heads - 4, lambda i: move("q", 2, i + 4).start())
        when(0, moved, stage_a)
        when(lag_b, lag_b + moved, stage_b)
        when(lag_c, lag_c + moved, stage_c)
        when(lag_d, lag_d + moved, lambda i: stage_back(0, i))
        when(lag_e, lag_e + moved, lambda i: stage_back(1, i))
        when(lag_f, lag_f + moved, lambda i: stage_back(2, i))

        def last_heads(i):
            h = i + moved
            move("q", 2, h).wait_recv()
            for hop in range(SECTIONS):
                row_move(hop, h).wait_recv()
            key_side(h)

        when(moved + lead, heads + lead, last_heads)

    @each(0, heads)
    def _(h):
        for hop in range(SECTIONS):
            row_move(hop, h).wait_send()
            move("q", hop, h).wait_send()

    @each(0, moved)
    def _(h):
        for hop in range(SECTIONS):
            stat_move(hop, h).wait_send()
            back_move(hop, h).wait_send()

    @each(moved, heads)
    def _(h):
        for hop in range(SECTIONS):
            for kind in "kv":
                move(kind, hop, h).wait_send()

    for hop in range(SECTIONS):
        og_move(hop).wait_send()
    for slot in range(SECTIONS + 1):
        for which in range(3):
            near(slot, which).wait_send()


def body(queries, key_rows, value_rows, out_grad, out_proj, section_table, block_active):
    seq_count = lax.axis_size("seq")
    heads = queries.shape[1] // HDIM
    moved = heads // 2
    width = queries.shape[1]
    part = moved * HDIM
    four = (SECTIONS + 1, BLK, width)
    any_space = pl.BlockSpec(memory_space=pl.ANY)
    vmem = pl.BlockSpec(memory_space=pltpu.VMEM)
    smem = pl.BlockSpec(memory_space=pltpu.SMEM)
    out = jax.ShapeDtypeStruct((BLK, width), jnp.bfloat16)
    bf16, f32, dma = jnp.bfloat16, jnp.float32, pltpu.SemaphoreType.DMA
    return pl.pallas_call(
        functools.partial(kernel, seq_count, moved),
        out_shape=(out, out, out),
        in_specs=[smem, smem] + [any_space] * 5,
        out_specs=(vmem, vmem, vmem),
        scratch_shapes=[
            pltpu.VMEM(four, bf16),
            pltpu.VMEM(four, bf16),
            pltpu.VMEM(four, bf16),
            pltpu.VMEM(four, bf16),
            pltpu.VMEM((SECTIONS + 1, 4, *out_grad.shape), bf16),
            pltpu.VMEM(out_proj.shape, bf16),
            pltpu.VMEM((SECTIONS + 1, BLK, BLK), f32),
            pltpu.VMEM((SECTIONS + 1, BLK, BLK), f32),
            pltpu.VMEM((SECTIONS + 1, moved, BLK, BLK), f32),
            pltpu.VMEM((SECTIONS + 1, moved, BLK, BLK), f32),
            pltpu.VMEM((SECTIONS + 1, moved, 8, BLK), f32),
            pltpu.VMEM((moved, 8, BLK), f32),
            pltpu.VMEM((BLK, width), f32),
            pltpu.VMEM((BLK, width), f32),
            pltpu.VMEM((SECTIONS, BLK, part), f32),
            pltpu.VMEM((SECTIONS, moved, 4, BLK), f32),
            pltpu.VMEM((SECTIONS, moved, 4, BLK), f32),
            pltpu.VMEM((SECTIONS, heads, 2, BLK), f32),
            pltpu.VMEM((SECTIONS, heads, 2, BLK), f32),
            pltpu.VMEM((SECTIONS, BLK, part), bf16),
            pltpu.VMEM((SECTIONS, BLK, part), bf16),
            dma((5,)),
            dma((SECTIONS,)),
            dma((SECTIONS,)),
            dma((SECTIONS + 1, 3)),
            dma((SECTIONS + 1, 3)),
            dma((3, SECTIONS, heads)),
            dma((3, SECTIONS, heads)),
            dma((SECTIONS, moved)),
            dma((SECTIONS, moved)),
            dma((SECTIONS, heads)),
            dma((SECTIONS, heads)),
            dma((SECTIONS, moved)),
            dma((SECTIONS, moved)),
        ],
        compiler_params=pltpu.CompilerParams(
            collective_id=0, has_side_effects=True, vmem_limit_bytes=60 * 1024 * 1024
        ),
        name="attention_grads",
    )(section_table.T, block_active, queries, key_rows, value_rows, out_grad, out_proj)


def solution(mesh):
    return jax.shard_map(
        body,
        mesh=mesh,
        in_specs=(
            P("seq", "head"),
            P("seq", "head"),
            P("seq", "head"),
            P("seq", "head"),
            P("head", None),
            P("head", None),
            P("seq", None),
        ),
        out_specs=(P("seq", "head"), P("seq", "head"), P("seq", "head")),
        check_vma=False,
    )
```

```python
import functools
import math

import jax
import jax.numpy as jnp
from jax import lax
from jax.experimental import pallas as pl
from jax.experimental.pallas import tpu as pltpu
from jax.sharding import PartitionSpec as P

BLK = 256
HDIM = 128
SECTIONS = 3
MESH = pl.DeviceIdType.MESH
HIDE = -1e30
SCALE = 1.0 / math.sqrt(HDIM)
NT = (((1,), (1,)), ((), ()))
TN = (((0,), (0,)), ((), ()))
NN = (((1,), (0,)), ((), ()))


def mm(a, b, dims):
    return lax.dot_general(a, b, dims, preferred_element_type=jnp.float32)


def kernel(
    seq_count, moved, table, active, q_in, k_in, v_in, og_in, w_in, dq, dk, dv,
    qa, ga, ka, va, og, w, scores, slopes, held_p, held_s, tops, norms, own_dk, own_dv, parts,
    stat_out, stat_in, row_out, row_in, back_out, back_in,
    local_sem, og_send, og_recv, near_send, near_recv, bulk_send, bulk_recv,
    stat_send, stat_recv, row_send, row_recv, back_send, back_recv,
):
    heads = q_in.shape[1] // HDIM
    width = og_in.shape[1]
    seq = lax.axis_index("seq")
    me = lax.axis_index("head")
    stride = seq_count // 8
    mates = (me, me + 1 - 2 * (me % 2), me + 2 - 4 * (me // 2), 3 - me)

    def along(steps):
        return {"seq": lax.rem(seq + (steps % 8) * stride, seq_count)}

    def cols(h):
        if isinstance(h, int):
            return pl.ds(h * HDIM, HDIM)
        return pl.ds(pl.multiple_of(h * HDIM, HDIM), HDIM)

    def remote(source, target, send, recv, device):
        return pltpu.make_async_remote_copy(
            src_ref=source, dst_ref=target, send_sem=send, recv_sem=recv,
            device_id=device, device_id_type=MESH,
        )

    bulk = {"k": (ka, 0, 1), "v": (va, 1, 1), "q": (qa, 2, -1)}

    def move(kind, hop, h):
        ref, row, sign = bulk[kind]
        return remote(
            ref.at[hop, :, cols(h)], ref.at[hop + 1, :, cols(h)],
            bulk_send.at[row, hop, h], bulk_recv.at[row, hop, h],
            along(sign * (2 if hop == 2 else 1)),
        )

    def half_of(half):
        return pl.ds(half * (width // 2), width // 2)

    def og_move(hop, half):
        part = half_of(half)
        return remote(
            og.at[hop, 0, :, part], og.at[hop + 1, 0, :, part],
            og_send.at[hop, half], og_recv.at[hop, half], along(-(2 if hop == 2 else 1)),
        )

    def near(slot, which, half):
        source, target, mate = ((0, 1, 1), (0, 2, 2), (2, 3, 1))[which]
        part = half_of(half)
        return remote(
            og.at[slot, source, :, part], og.at[slot, target, :, part],
            near_send.at[slot, which, half], near_recv.at[slot, which, half],
            {"head": mates[mate]},
        )

    def spread(slot, half):
        near(slot, 1, half).start()
        near(slot, 0, half).start()

    def stat_move(hop, h):
        return remote(
            stat_out.at[hop, h], stat_in.at[hop, h], stat_send.at[hop, h], stat_recv.at[hop, h],
            along((1, 2, 4)[hop]),
        )

    def row_move(hop, h):
        return remote(
            row_out.at[hop, h], row_in.at[hop, h], row_send.at[hop, h], row_recv.at[hop, h],
            along(-(1, 2, 4)[hop]),
        )

    def back_move(hop, h):
        return remote(
            back_out.at[hop, :, cols(h)], back_in.at[hop, :, cols(h)],
            back_send.at[hop, h], back_recv.at[hop, h], along((2, 1, 1)[hop]),
        )

    def hidden(hop, h):
        index = SECTIONS - 1 - hop
        inside = (seq >= seq_count // 2 ** (index + 1)).astype(jnp.int32)
        usable = table[index, h] * active[0, index] * inside
        return (1.0 - usable.astype(jnp.float32)) * HIDE

    def causal(raw):
        key_index = lax.broadcasted_iota(jnp.int32, (BLK, BLK), 0)
        query_index = lax.broadcasted_iota(jnp.int32, (BLK, BLK), 1)
        return jnp.where(key_index <= query_index, raw, HIDE)

    def make_grad(slot):
        for half in range(2):
            near(slot, 0, half).wait_recv()
            near(slot, 2, half).wait_recv()

        @pl.loop(0, heads // 2)
        def _(pair):
            wide = pl.ds(pl.multiple_of(pair * 2 * HDIM, 2 * HDIM), 2 * HDIM)
            total = jnp.zeros((BLK, 2 * HDIM), jnp.float32)
            for index, owner in enumerate(mates):
                features = pl.ds(pl.multiple_of(owner * width, width), width)
                total = total + mm(og[slot, index], w[wide, features], NT)
            ga[slot, :, wide] = total.astype(jnp.bfloat16)

    def pass_near(slot):
        for half in range(2):
            near(slot, 1, half).wait_recv()
            near(slot, 2, half).start()

    def pass_og(hop, half):
        og_move(hop, half).wait_recv()
        if hop < 2:
            og_move(hop + 1, half).start()
        spread(hop + 1, half)

    def query_side(h):
        at = cols(h)
        query = qa[0, :, at]
        grad = ga[0, :, at]
        top = None
        for s in range(SECTIONS + 1):
            raw = mm(ka[s, :, at], query, NT) * SCALE
            raw = causal(raw) if s == 0 else raw + hidden(s - 1, h)
            scores[s] = raw
            high = jnp.max(raw, axis=0, keepdims=True)
            top = high if top is None else jnp.maximum(top, high)
        total = None
        for s in range(SECTIONS + 1):
            part = jnp.exp(scores[s] - top)
            scores[s] = part
            part = jnp.sum(part, axis=0, keepdims=True)
            total = part if total is None else total + part
        inverse = 1.0 / total
        delta = None
        for s in range(SECTIONS + 1):
            probs = scores[s] * inverse
            scores[s] = probs
            weights = probs.astype(jnp.bfloat16)
            slope = mm(va[s, :, at], grad, NT)
            slopes[s] = slope
            part = jnp.sum(weights.astype(jnp.float32) * slope, axis=0, keepdims=True)
            delta = part if delta is None else delta + part
            if s == 0:
                own_dv[:, at] = mm(weights, grad, NN)
        log_norm = top + jnp.log(total)
        for hop in range(SECTIONS):
            row_out[hop, h, 0:1, :] = log_norm - hidden(hop, h)
            row_out[hop, h, 1:2, :] = delta
        query_sum = None
        for s in range(SECTIONS + 1):
            dlogit = (scores[s] * (slopes[s] - delta) * SCALE).astype(jnp.bfloat16)
            part = mm(dlogit, ka[s, :, at], TN)
            query_sum = part if query_sum is None else query_sum + part
            if s == 0:
                own_dk[:, at] = mm(dlogit, query, NN)
        dq[:, at] = query_sum.astype(jnp.bfloat16)
        for hop in range(SECTIONS):
            row_move(hop, h).start()

    def key_side(h):
        at = cols(h)
        key = ka[0, :, at]
        value = va[0, :, at]
        key_sum = own_dk[:, at]
        value_sum = own_dv[:, at]
        for hop in range(SECTIONS):
            query = qa[hop + 1, :, at]
            grad = ga[hop + 1, :, at]
            log_norm = row_in[hop, h, 0:1, :]
            delta = row_in[hop, h, 1:2, :]
            probs = jnp.exp(mm(key, query, NT) * SCALE - log_norm)
            slope = mm(value, grad, NT)
            dlogit = (probs * (slope - delta) * SCALE).astype(jnp.bfloat16)
            key_sum = key_sum + mm(dlogit, query, NN)
            value_sum = value_sum + mm(probs.astype(jnp.bfloat16), grad, NN)
        dk[:, at] = key_sum.astype(jnp.bfloat16)
        dv[:, at] = value_sum.astype(jnp.bfloat16)

    def partial_scores(slot, h):
        at = cols(h)
        raw = mm(ka[0, :, at], qa[slot, :, at], NT) * SCALE
        if slot == 0:
            raw = causal(raw)
        top = jnp.max(raw, axis=0, keepdims=True)
        part = jnp.exp(raw - top)
        slope = mm(va[0, :, at], ga[slot, :, at], NT)
        held_p[slot, h] = part
        held_s[slot, h] = slope
        total = jnp.sum(part, axis=0, keepdims=True)
        drift = jnp.sum(part * slope, axis=0, keepdims=True)
        tops[slot, h, 0:1, :] = top
        return top, total, drift

    def stage_own(h):
        top, total, drift = partial_scores(0, h)
        norms[h, 0:1, :] = total
        norms[h, 1:2, :] = drift

    def stage_a(h):
        for kind in ("q",):
            move(kind, 2, h).wait_recv()
        for hop in range(SECTIONS):
            top, total, drift = partial_scores(hop + 1, h)
            stat_out[hop, h, 0:1, :] = top
            stat_out[hop, h, 1:2, :] = total
            stat_out[hop, h, 2:3, :] = drift
            stat_out[hop, h, 3:4, :] = drift
            stat_move(hop, h).start()

    def stage_b(h):
        for hop in range(SECTIONS):
            stat_move(hop, h).wait_recv()
        tops_of = [tops[0, h, 0:1, :]] + [
            stat_in[hop, h, 0:1, :] + hidden(hop, h) for hop in range(SECTIONS)
        ]
        top = functools.reduce(jnp.maximum, tops_of)
        factor = jnp.exp(tops_of[0] - top)
        total = factor * norms[h, 0:1, :]
        drift = factor * norms[h, 1:2, :]
        for hop in range(SECTIONS):
            factor = jnp.exp(tops_of[hop + 1] - top)
            total = total + factor * stat_in[hop, h, 1:2, :]
            drift = drift + factor * stat_in[hop, h, 2:3, :]
        log_norm = top + jnp.log(total)
        delta = drift / total
        norms[h, 0:1, :] = log_norm
        norms[h, 1:2, :] = delta
        for hop in range(SECTIONS):
            row_out[hop, h, 0:1, :] = log_norm - hidden(hop, h)
            row_out[hop, h, 1:2, :] = delta
            row_move(hop, h).start()

    def stage_c(h):
        at = cols(h)
        for hop in range(SECTIONS):
            row_move(hop, h).wait_recv()
        key_sum = None
        value_sum = None
        for slot in (3, 2, 1, 0):
            if slot == 0:
                log_norm, delta = norms[h, 0:1, :], norms[h, 1:2, :]
            else:
                log_norm, delta = row_in[slot - 1, h, 0:1, :], row_in[slot - 1, h, 1:2, :]
            probs = held_p[slot, h] * jnp.exp(tops[slot, h, 0:1, :] - log_norm)
            dlogit = (probs * (held_s[slot, h] - delta) * SCALE).astype(jnp.bfloat16)
            query_part = mm(dlogit, ka[0, :, at], TN)
            if slot == 3:
                back_out[0, :, at] = query_part.astype(jnp.bfloat16)
            else:
                parts[slot, :, at] = query_part
            key_part = mm(dlogit, qa[slot, :, at], NN)
            value_part = mm(probs.astype(jnp.bfloat16), ga[slot, :, at], NN)
            key_sum = key_part if key_sum is None else key_sum + key_part
            value_sum = value_part if value_sum is None else value_sum + value_part
        dk[:, at] = key_sum.astype(jnp.bfloat16)
        dv[:, at] = value_sum.astype(jnp.bfloat16)
        back_move(0, h).start()

    def stage_back(hop, h):
        at = cols(h)
        back_move(hop, h).wait_recv()
        total = (parts[2 - hop, :, at] + back_in[hop, :, at].astype(jnp.float32)).astype(jnp.bfloat16)
        if hop == 2:
            dq[:, at] = total
        else:
            back_out[hop + 1, :, at] = total
            back_move(hop + 1, h).start()

    copies = [
        pltpu.make_async_copy(source, target, local_sem.at[index])
        for index, (source, target) in enumerate(
            ((og_in, og.at[0, 0]), (q_in, qa.at[0]), (k_in, ka.at[0]), (v_in, va.at[0]), (w_in, w))
        )
    ]
    for copy in copies:
        copy.start()

    barrier = pltpu.get_barrier_semaphore()
    for steps in (1, -1, 2, -2, 4):
        pl.semaphore_signal(barrier, inc=1, device_id=along(steps), device_id_type=MESH)
    for mate in mates[1:3]:
        pl.semaphore_signal(barrier, inc=1, device_id={"head": mate}, device_id_type=MESH)
    pl.semaphore_wait(barrier, 7)

    def each(first, last):
        return pl.loop(first, last)

    def begin(kinds, hop, first, last):
        @each(first, last)
        def _(h):
            for kind in kinds:
                move(kind, hop, h).start()

    def relay(kind, hop, h):
        move(kind, hop, h).wait_recv()
        move(kind, hop + 1, h).start()

    def late_query_side(h):
        move("k", 2, h).wait_recv()
        move("v", 2, h).wait_recv()
        query_side(h)

    def late_key_side(h):
        move("q", 2, h).wait_recv()
        for hop in range(SECTIONS):
            row_move(hop, h).wait_recv()
        key_side(h)

    def relay_kv(hop, h):
        relay("k", hop, h)
        relay("v", hop, h)

    copies[0].wait()
    for half in range(2):
        og_move(0, half).start()
    for half in range(2):
        spread(0, half)
    copies[2].wait()
    copies[3].wait()
    begin("kv", 0, moved, heads)
    copies[1].wait()
    pass_og(0, 0)
    pass_og(0, 1)
    begin("q", 0, 0, moved)
    relay_kv(0, 4)
    relay_kv(0, 5)
    pass_og(1, 0)
    relay_kv(0, 6)
    pass_og(1, 1)
    relay_kv(0, 7)
    pass_near(0)
    copies[4].wait()
    make_grad(0)
    for h in range(moved):
        relay("q", 0, h)
    pass_near(1)
    make_grad(1)
    relay_kv(1, 4)
    relay_kv(1, 5)
    pass_near(2)
    make_grad(2)
    relay_kv(1, 6)
    pass_og(2, 0)
    for h in range(moved):
        stage_own(h)
    pass_og(2, 1)
    late_query_side(4)
    for h in range(moved):
        relay("q", 1, h)
    late_query_side(5)
    pass_near(3)
    make_grad(3)
    stage_a(0)
    stage_a(1)
    relay_kv(1, 7)
    late_query_side(6)
    stage_b(0)
    begin("q", 0, 4, 6)
    stage_a(2)
    stage_b(1)
    begin("q", 0, 6, 8)
    stage_a(3)
    late_query_side(7)
    stage_b(2)
    relay("q", 0, 4)
    stage_c(0)
    relay("q", 0, 5)
    stage_c(1)
    stage_b(3)
    relay("q", 0, 6)
    relay("q", 0, 7)
    stage_c(2)
    stage_back(0, 0)
    relay("q", 1, 4)
    stage_c(3)
    relay("q", 1, 5)
    stage_back(0, 1)
    relay("q", 1, 6)
    stage_back(1, 0)
    stage_back(0, 2)
    relay("q", 1, 7)
    stage_back(1, 1)
    late_key_side(4)
    stage_back(0, 3)
    stage_back(2, 0)
    stage_back(1, 2)
    late_key_side(5)
    stage_back(2, 1)
    stage_back(1, 3)
    late_key_side(6)
    stage_back(2, 2)
    late_key_side(7)
    stage_back(2, 3)

    @each(0, heads)
    def _(h):
        for hop in range(SECTIONS):
            row_move(hop, h).wait_send()
            move("q", hop, h).wait_send()

    @each(0, moved)
    def _(h):
        for hop in range(SECTIONS):
            stat_move(hop, h).wait_send()
            back_move(hop, h).wait_send()

    @each(moved, heads)
    def _(h):
        for hop in range(SECTIONS):
            for kind in "kv":
                move(kind, hop, h).wait_send()

    for half in range(2):
        for hop in range(SECTIONS):
            og_move(hop, half).wait_send()
        for slot in range(SECTIONS + 1):
            for which in range(3):
                near(slot, which, half).wait_send()


def write_out(dq, dk, dv, dq_out, dk_out, dv_out, sem):
    copies = [
        pltpu.make_async_copy(source, target, sem.at[index])
        for index, (source, target) in enumerate(((dq, dq_out), (dk, dk_out), (dv, dv_out)))
    ]
    for copy in copies:
        copy.start()
    for copy in copies:
        copy.wait()


def body(queries, key_rows, value_rows, out_grad, out_proj, section_table, block_active):
    seq_count = lax.axis_size("seq")
    heads = queries.shape[1] // HDIM
    moved = heads // 2
    width = queries.shape[1]
    part = moved * HDIM
    four = (SECTIONS + 1, BLK, width)
    any_space = pl.BlockSpec(memory_space=pl.ANY)
    vmem = pl.BlockSpec(memory_space=pltpu.VMEM)
    smem = pl.BlockSpec(memory_space=pltpu.SMEM)
    out = jax.ShapeDtypeStruct((BLK, width), jnp.bfloat16)
    bf16, f32, dma = jnp.bfloat16, jnp.float32, pltpu.SemaphoreType.DMA
    placed = [
        pltpu.with_memory_space_constraint(array, pltpu.HBM)
        for array in (
            section_table.T, block_active, queries, key_rows, value_rows, out_grad, out_proj
        )
    ]
    grads = pl.pallas_call(
        functools.partial(kernel, seq_count, moved),
        out_shape=(out, out, out),
        in_specs=[smem, smem] + [pl.BlockSpec(memory_space=pltpu.HBM)] * 5,
        out_specs=(vmem, vmem, vmem),
        scratch_shapes=[
            pltpu.VMEM(four, bf16),
            pltpu.VMEM(four, bf16),
            pltpu.VMEM(four, bf16),
            pltpu.VMEM(four, bf16),
            pltpu.VMEM((SECTIONS + 1, 4, *out_grad.shape), bf16),
            pltpu.VMEM(out_proj.shape, bf16),
            pltpu.VMEM((SECTIONS + 1, BLK, BLK), f32),
            pltpu.VMEM((SECTIONS + 1, BLK, BLK), f32),
            pltpu.VMEM((SECTIONS + 1, moved, BLK, BLK), f32),
            pltpu.VMEM((SECTIONS + 1, moved, BLK, BLK), f32),
            pltpu.VMEM((SECTIONS + 1, moved, 8, BLK), f32),
            pltpu.VMEM((moved, 8, BLK), f32),
            pltpu.VMEM((BLK, width), f32),
            pltpu.VMEM((BLK, width), f32),
            pltpu.VMEM((SECTIONS, BLK, part), f32),
            pltpu.VMEM((SECTIONS, moved, 4, BLK), f32),
            pltpu.VMEM((SECTIONS, moved, 4, BLK), f32),
            pltpu.VMEM((SECTIONS, heads, 2, BLK), f32),
            pltpu.VMEM((SECTIONS, heads, 2, BLK), f32),
            pltpu.VMEM((SECTIONS, BLK, part), bf16),
            pltpu.VMEM((SECTIONS, BLK, part), bf16),
            dma((5,)),
            dma((SECTIONS, 2)),
            dma((SECTIONS, 2)),
            dma((SECTIONS + 1, 3, 2)),
            dma((SECTIONS + 1, 3, 2)),
            dma((3, SECTIONS, heads)),
            dma((3, SECTIONS, heads)),
            dma((SECTIONS, moved)),
            dma((SECTIONS, moved)),
            dma((SECTIONS, heads)),
            dma((SECTIONS, heads)),
            dma((SECTIONS, moved)),
            dma((SECTIONS, moved)),
        ],
        compiler_params=pltpu.CompilerParams(
            collective_id=0, has_side_effects=True, vmem_limit_bytes=44 * 1024 * 1024
        ),
        name="attention_grads",
    )(*placed)
    return pl.pallas_call(
        write_out,
        out_shape=(out, out, out),
        in_specs=[vmem] * 3,
        out_specs=[any_space] * 3,
        scratch_shapes=[dma((3,))],
        compiler_params=pltpu.CompilerParams(vmem_limit_bytes=4 * 1024 * 1024),
        name="write_out",
    )(*grads)


def solution(mesh):
    return jax.shard_map(
        body,
        mesh=mesh,
        in_specs=(
            P("seq", "head"),
            P("seq", "head"),
            P("seq", "head"),
            P("seq", "head"),
            P("head", None),
            P("head", None),
            P("seq", None),
        ),
        out_specs=(P("seq", "head"), P("seq", "head"), P("seq", "head")),
        check_vma=False,
    )
```

```python
import functools
import math

import jax
import jax.numpy as jnp
from jax import lax
from jax.experimental import pallas as pl
from jax.experimental.pallas import tpu as pltpu
from jax.sharding import PartitionSpec as P

BLK = 256
HDIM = 128
SECTIONS = 3
PARTS = 4
MODE = "open"
KV_WRAP = True
OG_WRAP = True
MESH = pl.DeviceIdType.MESH
HIDE = -1e30
SCALE = 1.0 / math.sqrt(HDIM)
NT = (((1,), (1,)), ((), ()))
TN = (((0,), (0,)), ((), ()))
NN = (((1,), (0,)), ((), ()))


def given(condition):
    if isinstance(condition, bool):
        return (lambda action: action()) if condition else (lambda action: None)
    return pl.when(condition)


def opposite(condition):
    return not condition if isinstance(condition, bool) else jnp.logical_not(condition)


def mm(a, b, dims):
    return lax.dot_general(a, b, dims, preferred_element_type=jnp.float32)


def kernel(
    seq_count, moved, table, active, q_in, k_in, v_in, og_in, w_in, dq, dk, dv,
    qa, ga, ka, va, og, og_wrap, kv_wrap, w, scores, slopes, held_p, held_s, tops, norms, own_dk, own_dv, parts,
    stat_out, stat_in, row_out, row_in, back_out, back_in,
    local_sem, og_send, og_recv, hop_send, hop_recv, wrap_send, wrap_recv, near_send, near_recv, bulk_send, bulk_recv,
    stat_send, stat_recv, row_send, row_recv, back_send, back_recv,
):
    heads = q_in.shape[1] // HDIM
    width = og_in.shape[1]
    seq = lax.axis_index("seq")
    me = lax.axis_index("head")
    stride = seq_count // 8
    z = seq // stride
    far = (1, 2, 4)
    if MODE == "cyclic":
        above = below = [True] * 3
        down_send = up_send = og_sends = back_send_if = back_recv_if = (True, True, True)
    else:
        above = [z + steps <= 7 for steps in far]
        below = [z >= steps for steps in far]
        middle = (z >= 2) & (z <= 5)
        down_send = (z >= 1, (z >= 1) & (z <= 6), middle)
        up_send = (z <= 6, (z >= 1) & (z <= 6), (z == 2) | (z == 4) | (z == 5) if KV_WRAP else middle)
        og_sends = (z >= 1, (z >= 1) & (z <= 6), (z == 2) | (z == 5) if OG_WRAP else middle)
        back_send_if = (z <= 3, z <= 5, z <= 6)
        back_recv_if = (middle, (z >= 1) & (z <= 6), z >= 1)
    og_forward = (z == 7) | (z == 0) if OG_WRAP else False
    og_leaves = (z == 5) | (z == 6) if OG_WRAP else False
    kv_leaves = z == 1 if KV_WRAP else False
    kv_forward = z == 7 if KV_WRAP else False
    mates = (me, me + 1 - 2 * (me % 2), me + 2 - 4 * (me // 2), 3 - me)

    def along(steps):
        return {"seq": lax.rem(seq + (steps % 8) * stride, seq_count)}

    def cols(h):
        if isinstance(h, int):
            return pl.ds(h * HDIM, HDIM)
        return pl.ds(pl.multiple_of(h * HDIM, HDIM), HDIM)

    def remote(source, target, send, recv, device):
        return pltpu.make_async_remote_copy(
            src_ref=source, dst_ref=target, send_sem=send, recv_sem=recv,
            device_id=device, device_id_type=MESH,
        )

    bulk = {"k": (ka, 0, 1), "v": (va, 1, 1), "q": (qa, 2, -1)}

    def move(kind, hop, h):
        ref, row, sign = bulk[kind]
        return remote(
            ref.at[hop, :, cols(h)], ref.at[hop + 1, :, cols(h)],
            bulk_send.at[row, hop, h], bulk_recv.at[row, hop, h],
            along(sign * (2 if hop == 2 else 1)),
        )

    def half_of(half):
        return pl.ds(half * (width // PARTS), width // PARTS)

    def og_move(hop, half):
        part = half_of(half)
        return remote(
            og.at[hop, 0, :, part], og.at[hop + 1, 0, :, part],
            og_send.at[hop, half], og_recv.at[hop, half], along(-(2 if hop == 2 else 1)),
        )

    def og_out(half):
        part = half_of(half)
        return remote(
            og.at[0, 0, :, part], og_wrap.at[:, part],
            hop_send.at[half], hop_recv.at[half], along(2),
        )

    def og_on(half):
        part = half_of(half)
        return remote(
            og_wrap.at[:, part], og.at[3, 0, :, part],
            og_send.at[2, half], og_recv.at[2, half], along(2),
        )

    def kv_out(index, h):
        ref = (ka, va)[index]
        return remote(
            ref.at[0, :, cols(h)], kv_wrap.at[index, :, cols(h - moved)],
            wrap_send.at[index, h], wrap_recv.at[index, h], along(-2),
        )

    def kv_on(index, h):
        ref = (ka, va)[index]
        return remote(
            kv_wrap.at[index, :, cols(h - moved)], ref.at[3, :, cols(h)],
            bulk_send.at[index, 2, h], bulk_recv.at[index, 2, h], along(-2),
        )

    def sends(kind, hop):
        return (down_send if kind == "q" else up_send)[hop]

    def comes(kind, hop):
        return (above if kind == "q" else below)[hop]

    def started(condition, copy):
        @given(condition)
        def _():
            copy().start()

    def landed(condition, copy):
        @given(condition)
        def _():
            copy().wait_recv()

    def left(condition, copy):
        @given(condition)
        def _():
            copy().wait_send()

    def near(slot, which, half):
        source, target, mate = ((0, 1, 1), (0, 2, 2), (2, 3, 1))[which]
        part = half_of(half)
        return remote(
            og.at[slot, source, :, part], og.at[slot, target, :, part],
            near_send.at[slot, which, half], near_recv.at[slot, which, half],
            {"head": mates[mate]},
        )

    def spread(slot, half):
        near(slot, 1, half).start()
        near(slot, 0, half).start()

    def stat_move(hop, h):
        return remote(
            stat_out.at[hop, h], stat_in.at[hop, h], stat_send.at[hop, h], stat_recv.at[hop, h],
            along((1, 2, 4)[hop]),
        )

    def row_move(hop, h):
        return remote(
            row_out.at[hop, h], row_in.at[hop, h], row_send.at[hop, h], row_recv.at[hop, h],
            along(-(1, 2, 4)[hop]),
        )

    def back_move(hop, h):
        return remote(
            back_out.at[hop, :, cols(h)], back_in.at[hop, :, cols(h)],
            back_send.at[hop, h], back_recv.at[hop, h], along((2, 1, 1)[hop]),
        )

    def hidden(hop, h):
        index = SECTIONS - 1 - hop
        inside = (seq >= seq_count // 2 ** (index + 1)).astype(jnp.int32)
        usable = table[index, h] * active[0, index] * inside
        return (1.0 - usable.astype(jnp.float32)) * HIDE

    def causal(raw):
        key_index = lax.broadcasted_iota(jnp.int32, (BLK, BLK), 0)
        query_index = lax.broadcasted_iota(jnp.int32, (BLK, BLK), 1)
        return jnp.where(key_index <= query_index, raw, HIDE)

    def slot_used(slot):
        return True if slot == 0 else above[slot - 1]

    def make_grad(slot):
        @given(slot_used(slot))
        def _():
            for half in range(PARTS):
                near(slot, 0, half).wait_recv()
                near(slot, 2, half).wait_recv()

            @pl.loop(0, heads // 2)
            def _(pair):
                wide = pl.ds(pl.multiple_of(pair * 2 * HDIM, 2 * HDIM), 2 * HDIM)
                total = jnp.zeros((BLK, 2 * HDIM), jnp.float32)
                for index, owner in enumerate(mates):
                    features = pl.ds(pl.multiple_of(owner * width, width), width)
                    total = total + mm(og[slot, index], w[wide, features], NT)
                ga[slot, :, wide] = total.astype(jnp.bfloat16)

    def pass_near(slot):
        @given(slot_used(slot))
        def _():
            for half in range(PARTS):
                near(slot, 1, half).wait_recv()
                near(slot, 2, half).start()

    def pass_og(hop, half):
        @given(above[hop])
        def _():
            og_move(hop, half).wait_recv()
        if hop < 2:
            started(og_sends[hop + 1], lambda: og_move(hop + 1, half))
        @given(above[hop])
        def _():
            spread(hop + 1, half)

    def forward_og(half):
        @given(og_forward)
        def _():
            og_out(half).wait_recv()
            og_on(half).start()

    def forward_kv(h):
        @given(kv_forward)
        def _():
            for index in range(2):
                kv_out(index, h).wait_recv()
                kv_on(index, h).start()

    def query_side(h):
        at = cols(h)
        query = qa[0, :, at]
        grad = ga[0, :, at]
        top = None
        for s in range(SECTIONS + 1):
            raw = mm(ka[s, :, at], query, NT) * SCALE
            raw = causal(raw) if s == 0 else raw + hidden(s - 1, h)
            scores[s] = raw
            high = jnp.max(raw, axis=0, keepdims=True)
            top = high if top is None else jnp.maximum(top, high)
        total = None
        for s in range(SECTIONS + 1):
            part = jnp.exp(scores[s] - top)
            scores[s] = part
            part = jnp.sum(part, axis=0, keepdims=True)
            total = part if total is None else total + part
        inverse = 1.0 / total
        delta = None
        for s in range(SECTIONS + 1):
            probs = scores[s] * inverse
            scores[s] = probs
            weights = probs.astype(jnp.bfloat16)
            slope = mm(va[s, :, at], grad, NT)
            slopes[s] = slope
            part = jnp.sum(weights.astype(jnp.float32) * slope, axis=0, keepdims=True)
            delta = part if delta is None else delta + part
            if s == 0:
                own_dv[:, at] = mm(weights, grad, NN)
        log_norm = top + jnp.log(total)
        for hop in range(SECTIONS):
            row_out[hop, h, 0:1, :] = log_norm - hidden(hop, h)
            row_out[hop, h, 1:2, :] = delta
        query_sum = None
        for s in range(SECTIONS + 1):
            dlogit = (scores[s] * (slopes[s] - delta) * SCALE).astype(jnp.bfloat16)
            part = mm(dlogit, ka[s, :, at], TN)
            query_sum = part if query_sum is None else query_sum + part
            if s == 0:
                own_dk[:, at] = mm(dlogit, query, NN)
        dq[:, at] = query_sum.astype(jnp.bfloat16)
        for hop in range(SECTIONS):
            started(below[hop], lambda hop=hop: row_move(hop, h))

    def key_side(h):
        at = cols(h)
        key = ka[0, :, at]
        value = va[0, :, at]
        key_sum = own_dk[:, at]
        value_sum = own_dv[:, at]
        for hop in range(SECTIONS):
            query = qa[hop + 1, :, at]
            grad = ga[hop + 1, :, at]
            log_norm = row_in[hop, h, 0:1, :]
            delta = row_in[hop, h, 1:2, :]
            probs = jnp.exp(mm(key, query, NT) * SCALE - log_norm)
            slope = mm(value, grad, NT)
            dlogit = (probs * (slope - delta) * SCALE).astype(jnp.bfloat16)
            key_sum = key_sum + mm(dlogit, query, NN)
            value_sum = value_sum + mm(probs.astype(jnp.bfloat16), grad, NN)
        dk[:, at] = key_sum.astype(jnp.bfloat16)
        dv[:, at] = value_sum.astype(jnp.bfloat16)

    def partial_scores(slot, h):
        at = cols(h)
        raw = mm(ka[0, :, at], qa[slot, :, at], NT) * SCALE
        if slot == 0:
            raw = causal(raw)
        top = jnp.max(raw, axis=0, keepdims=True)
        part = jnp.exp(raw - top)
        slope = mm(va[0, :, at], ga[slot, :, at], NT)
        held_p[slot, h] = part
        held_s[slot, h] = slope
        total = jnp.sum(part, axis=0, keepdims=True)
        drift = jnp.sum(part * slope, axis=0, keepdims=True)
        tops[slot, h, 0:1, :] = top
        return top, total, drift

    def stage_own(h):
        top, total, drift = partial_scores(0, h)
        norms[h, 0:1, :] = total
        norms[h, 1:2, :] = drift

    def stage_a(h):
        landed(comes("q", 2), lambda: move("q", 2, h))
        for hop in range(SECTIONS):
            top, total, drift = partial_scores(hop + 1, h)
            stat_out[hop, h, 0:1, :] = top
            stat_out[hop, h, 1:2, :] = total
            stat_out[hop, h, 2:3, :] = drift
            stat_out[hop, h, 3:4, :] = drift
            started(above[hop], lambda hop=hop: stat_move(hop, h))

    def stage_b(h):
        for hop in range(SECTIONS):
            landed(below[hop], lambda hop=hop: stat_move(hop, h))
        tops_of = [tops[0, h, 0:1, :]] + [
            stat_in[hop, h, 0:1, :] + hidden(hop, h) for hop in range(SECTIONS)
        ]
        top = functools.reduce(jnp.maximum, tops_of)
        factor = jnp.exp(tops_of[0] - top)
        total = factor * norms[h, 0:1, :]
        drift = factor * norms[h, 1:2, :]
        for hop in range(SECTIONS):
            factor = jnp.exp(tops_of[hop + 1] - top)
            total = total + factor * stat_in[hop, h, 1:2, :]
            drift = drift + factor * stat_in[hop, h, 2:3, :]
        log_norm = top + jnp.log(total)
        delta = drift / total
        norms[h, 0:1, :] = log_norm
        norms[h, 1:2, :] = delta
        for hop in range(SECTIONS):
            row_out[hop, h, 0:1, :] = log_norm - hidden(hop, h)
            row_out[hop, h, 1:2, :] = delta
            started(below[hop], lambda hop=hop: row_move(hop, h))

    def stage_c(h):
        at = cols(h)
        for hop in range(SECTIONS):
            landed(above[hop], lambda hop=hop: row_move(hop, h))
        key_sum = None
        value_sum = None
        for slot in (3, 2, 1, 0):
            if slot == 0:
                log_norm, delta = norms[h, 0:1, :], norms[h, 1:2, :]
            else:
                log_norm, delta = row_in[slot - 1, h, 0:1, :], row_in[slot - 1, h, 1:2, :]
            probs = held_p[slot, h] * jnp.exp(tops[slot, h, 0:1, :] - log_norm)
            dlogit = (probs * (held_s[slot, h] - delta) * SCALE).astype(jnp.bfloat16)
            query_part = mm(dlogit, ka[0, :, at], TN)
            if slot == 3:
                back_out[0, :, at] = query_part.astype(jnp.bfloat16)
            else:
                parts[slot, :, at] = query_part
            key_part = mm(dlogit, qa[slot, :, at], NN)
            value_part = mm(probs.astype(jnp.bfloat16), ga[slot, :, at], NN)
            key_sum = key_part if key_sum is None else key_sum + key_part
            value_sum = value_part if value_sum is None else value_sum + value_part
        dk[:, at] = key_sum.astype(jnp.bfloat16)
        dv[:, at] = value_sum.astype(jnp.bfloat16)
        started(back_send_if[0], lambda: back_move(0, h))

    def stage_back(hop, h):
        at = cols(h)
        landed(back_recv_if[hop], lambda: back_move(hop, h))
        total = (parts[2 - hop, :, at] + back_in[hop, :, at].astype(jnp.float32)).astype(jnp.bfloat16)
        if hop == 2:
            dq[:, at] = total
        else:
            back_out[hop + 1, :, at] = total
            started(back_send_if[hop + 1], lambda: back_move(hop + 1, h))

    copies = [
        pltpu.make_async_copy(source, target, local_sem.at[index])
        for index, (source, target) in enumerate(
            ((og_in, og.at[0, 0]), (q_in, qa.at[0]), (k_in, ka.at[0]), (v_in, va.at[0]), (w_in, w))
        )
    ]
    for copy in copies:
        copy.start()

    def fill(ref, value=0.0):
        ref[...] = jnp.full(ref.shape, value, ref.dtype)

    for slot in range(1, SECTIONS + 1):
        @given(opposite(above[slot - 1]))
        def _(slot=slot):
            fill(qa.at[slot])
            fill(ga.at[slot])
            fill(row_in.at[slot - 1], -HIDE)

        @given(opposite(below[slot - 1]))
        def _(slot=slot):
            fill(ka.at[slot])
            fill(va.at[slot])
            fill(stat_in.at[slot - 1])

        @given(opposite(back_recv_if[slot - 1]))
        def _(slot=slot):
            fill(back_in.at[slot - 1])

    barrier = pltpu.get_barrier_semaphore()
    for steps in (1, -1, 2, -2, 4):
        pl.semaphore_signal(barrier, inc=1, device_id=along(steps), device_id_type=MESH)
    for mate in mates[1:3]:
        pl.semaphore_signal(barrier, inc=1, device_id={"head": mate}, device_id_type=MESH)
    pl.semaphore_wait(barrier, 7)

    def each(first, last):
        return pl.loop(first, last)

    def begin(kinds, hop, first, last):
        @given(sends(kinds[0], hop))
        def _():
            @each(first, last)
            def _(h):
                for kind in kinds:
                    move(kind, hop, h).start()

    def relay(kind, hop, h):
        landed(comes(kind, hop), lambda: move(kind, hop, h))
        started(sends(kind, hop + 1), lambda: move(kind, hop + 1, h))

    def late_query_side(h):
        for kind in "kv":
            landed(comes(kind, 2), lambda kind=kind: move(kind, 2, h))
        query_side(h)

    def late_key_side(h):
        landed(comes("q", 2), lambda: move("q", 2, h))
        for hop in range(SECTIONS):
            landed(above[hop], lambda hop=hop: row_move(hop, h))
        key_side(h)

    def relay_kv(hop, h):
        relay("k", hop, h)
        relay("v", hop, h)

    def send_kv_round(first, last):
        @given(kv_leaves)
        def _():
            @each(first, last)
            def _(h):
                kv_out(0, h).start()
                kv_out(1, h).start()

    copies[0].wait()
    for half in range(PARTS):
        started(og_sends[0], lambda half=half: og_move(0, half))
    for half in range(PARTS):
        spread(0, half)
    for half in range(PARTS):
        started(og_leaves, lambda half=half: og_out(half))
    copies[2].wait()
    copies[3].wait()
    begin("kv", 0, moved, heads)
    copies[1].wait()
    pass_og(0, 0)
    pass_og(0, 1)
    pass_og(0, 2)
    pass_og(0, 3)
    begin("q", 0, 0, 4)
    pass_og(1, 0)
    forward_og(0)
    pass_og(1, 1)
    forward_og(1)
    relay_kv(0, 4)
    pass_og(1, 2)
    forward_og(2)
    pass_og(1, 3)
    forward_og(3)
    relay_kv(0, 5)
    relay_kv(0, 6)
    relay_kv(0, 7)
    pass_near(0)
    copies[4].wait()
    make_grad(0)
    pass_near(1)
    relay("q", 0, 0)
    relay("q", 0, 1)
    relay("q", 0, 2)
    relay("q", 0, 3)
    send_kv_round(4, 6)
    make_grad(1)
    pass_og(2, 0)
    pass_og(2, 1)
    stage_own(0)
    stage_own(1)
    stage_own(2)
    stage_own(3)
    pass_og(2, 2)
    pass_og(2, 3)
    pass_near(2)
    make_grad(2)
    relay("q", 1, 0)
    relay("q", 1, 1)
    relay("q", 1, 2)
    pass_near(3)
    make_grad(3)
    stage_a(0)
    relay_kv(1, 4)
    stage_a(1)
    relay("q", 1, 3)
    send_kv_round(6, 8)
    relay_kv(1, 5)
    forward_kv(4)
    stage_b(0)
    begin("q", 0, 4, 8)
    forward_kv(5)
    stage_a(2)
    relay_kv(1, 6)
    stage_b(1)
    stage_a(3)
    relay_kv(1, 7)
    forward_kv(6)
    relay("q", 0, 4)
    stage_b(2)
    relay("q", 0, 5)
    stage_c(0)
    stage_b(3)
    forward_kv(7)
    relay("q", 0, 6)
    stage_c(1)
    relay("q", 0, 7)
    late_query_side(4)
    relay("q", 1, 4)
    stage_back(0, 0)
    stage_c(2)
    relay("q", 1, 5)
    late_query_side(5)
    stage_c(3)
    stage_back(0, 1)
    relay("q", 1, 6)
    stage_back(1, 0)
    late_query_side(6)
    relay("q", 1, 7)
    stage_back(0, 2)
    stage_back(1, 1)
    late_query_side(7)
    stage_back(0, 3)
    stage_back(2, 0)
    stage_back(1, 2)
    late_key_side(4)
    stage_back(2, 1)
    stage_back(1, 3)
    late_key_side(5)
    stage_back(2, 2)
    late_key_side(6)
    stage_back(2, 3)
    late_key_side(7)

    @each(0, heads)
    def _(h):
        for hop in range(SECTIONS):
            left(below[hop], lambda hop=hop: row_move(hop, h))
            left(down_send[hop], lambda hop=hop: move("q", hop, h))

    @each(0, moved)
    def _(h):
        for hop in range(SECTIONS):
            left(above[hop], lambda hop=hop: stat_move(hop, h))
            left(back_send_if[hop], lambda hop=hop: back_move(hop, h))

    @each(moved, heads)
    def _(h):
        for hop in range(SECTIONS):
            for kind in "kv":
                left(up_send[hop], lambda kind=kind, hop=hop: move(kind, hop, h))
        for index in range(2):
            left(kv_leaves, lambda index=index: kv_out(index, h))
            left(kv_forward, lambda index=index: kv_on(index, h))

    for half in range(PARTS):
        left(og_leaves, lambda half=half: og_out(half))
        left(og_forward, lambda half=half: og_on(half))
        for hop in range(SECTIONS):
            left(og_sends[hop], lambda hop=hop, half=half: og_move(hop, half))
        for slot in range(SECTIONS + 1):
            for which in range(3):
                left(slot_used(slot), lambda slot=slot, which=which, half=half: near(slot, which, half))


def write_out(dq, dk, dv, dq_out, dk_out, dv_out, sem):
    copies = [
        pltpu.make_async_copy(source, target, sem.at[index])
        for index, (source, target) in enumerate(((dq, dq_out), (dk, dk_out), (dv, dv_out)))
    ]
    for copy in copies:
        copy.start()
    for copy in copies:
        copy.wait()


def body(queries, key_rows, value_rows, out_grad, out_proj, section_table, block_active):
    seq_count = lax.axis_size("seq")
    heads = queries.shape[1] // HDIM
    moved = heads // 2
    width = queries.shape[1]
    part = moved * HDIM
    four = (SECTIONS + 1, BLK, width)
    any_space = pl.BlockSpec(memory_space=pl.ANY)
    vmem = pl.BlockSpec(memory_space=pltpu.VMEM)
    smem = pl.BlockSpec(memory_space=pltpu.SMEM)
    out = jax.ShapeDtypeStruct((BLK, width), jnp.bfloat16)
    bf16, f32, dma = jnp.bfloat16, jnp.float32, pltpu.SemaphoreType.DMA
    placed = [
        pltpu.with_memory_space_constraint(array, pltpu.HBM)
        for array in (
            section_table.T, block_active, queries, key_rows, value_rows, out_grad, out_proj
        )
    ]
    grads = pl.pallas_call(
        functools.partial(kernel, seq_count, moved),
        out_shape=(out, out, out),
        in_specs=[smem, smem] + [pl.BlockSpec(memory_space=pltpu.HBM)] * 5,
        out_specs=(vmem, vmem, vmem),
        scratch_shapes=[
            pltpu.VMEM(four, bf16),
            pltpu.VMEM(four, bf16),
            pltpu.VMEM(four, bf16),
            pltpu.VMEM(four, bf16),
            pltpu.VMEM((SECTIONS + 1, 4, *out_grad.shape), bf16),
            pltpu.VMEM(out_grad.shape, bf16),
            pltpu.VMEM((2, BLK, width - part), bf16),
            pltpu.VMEM(out_proj.shape, bf16),
            pltpu.VMEM((SECTIONS + 1, BLK, BLK), f32),
            pltpu.VMEM((SECTIONS + 1, BLK, BLK), f32),
            pltpu.VMEM((SECTIONS + 1, moved, BLK, BLK), f32),
            pltpu.VMEM((SECTIONS + 1, moved, BLK, BLK), f32),
            pltpu.VMEM((SECTIONS + 1, moved, 8, BLK), f32),
            pltpu.VMEM((moved, 8, BLK), f32),
            pltpu.VMEM((BLK, width), f32),
            pltpu.VMEM((BLK, width), f32),
            pltpu.VMEM((SECTIONS, BLK, part), f32),
            pltpu.VMEM((SECTIONS, moved, 4, BLK), f32),
            pltpu.VMEM((SECTIONS, moved, 4, BLK), f32),
            pltpu.VMEM((SECTIONS, heads, 2, BLK), f32),
            pltpu.VMEM((SECTIONS, heads, 2, BLK), f32),
            pltpu.VMEM((SECTIONS, BLK, part), bf16),
            pltpu.VMEM((SECTIONS, BLK, part), bf16),
            dma((5,)),
            dma((SECTIONS, PARTS)),
            dma((SECTIONS, PARTS)),
            dma((PARTS,)),
            dma((PARTS,)),
            dma((2, heads)),
            dma((2, heads)),
            dma((SECTIONS + 1, 3, PARTS)),
            dma((SECTIONS + 1, 3, PARTS)),
            dma((3, SECTIONS, heads)),
            dma((3, SECTIONS, heads)),
            dma((SECTIONS, moved)),
            dma((SECTIONS, moved)),
            dma((SECTIONS, heads)),
            dma((SECTIONS, heads)),
            dma((SECTIONS, moved)),
            dma((SECTIONS, moved)),
        ],
        compiler_params=pltpu.CompilerParams(
            collective_id=0, has_side_effects=True, vmem_limit_bytes=44 * 1024 * 1024
        ),
        name="attention_grads",
    )(*placed)
    return pl.pallas_call(
        write_out,
        out_shape=(out, out, out),
        in_specs=[vmem] * 3,
        out_specs=[any_space] * 3,
        scratch_shapes=[dma((3,))],
        compiler_params=pltpu.CompilerParams(vmem_limit_bytes=4 * 1024 * 1024),
        name="write_out",
    )(*grads)


def solution(mesh):
    return jax.shard_map(
        body,
        mesh=mesh,
        in_specs=(
            P("seq", "head"),
            P("seq", "head"),
            P("seq", "head"),
            P("seq", "head"),
            P("head", None),
            P("head", None),
            P("seq", None),
        ),
        out_specs=(P("seq", "head"), P("seq", "head"), P("seq", "head")),
        check_vma=False,
    )
```

```python
import functools
import math

import jax
import jax.numpy as jnp
from jax import lax
from jax.experimental import pallas as pl
from jax.experimental.pallas import tpu as pltpu
from jax.sharding import PartitionSpec as P

BLK = 256
HDIM = 128
SECTIONS = 3
PARTS = 4
EARLY = 6
MODE = "open"
KV_WRAP = True
OG_WRAP = True
MESH = pl.DeviceIdType.MESH
HIDE = -1e30
SCALE = 1.0 / math.sqrt(HDIM)
NT = (((1,), (1,)), ((), ()))
TN = (((0,), (0,)), ((), ()))
NN = (((1,), (0,)), ((), ()))


def given(condition):
    if isinstance(condition, bool):
        return (lambda action: action()) if condition else (lambda action: None)
    return pl.when(condition)


def opposite(condition):
    return not condition if isinstance(condition, bool) else jnp.logical_not(condition)


def mm(a, b, dims):
    return lax.dot_general(a, b, dims, preferred_element_type=jnp.float32)


def kernel(
    seq_count, moved, table, active, q_in, k_in, v_in, og_in, w_in, dq, dk, dv,
    qa, ga, ka, va, og, og_wrap, kv_wrap, w, scores, slopes, held_p, held_s, tops, norms, own_dk, own_dv, parts,
    stat_out, stat_in, row_out, row_in, back_out, back_in,
    local_sem, og_send, og_recv, hop_send, hop_recv, wrap_send, wrap_recv, near_send, near_recv, bulk_send, bulk_recv,
    stat_send, stat_recv, row_send, row_recv, back_send, back_recv,
):
    heads = q_in.shape[1] // HDIM
    width = og_in.shape[1]
    seq = lax.axis_index("seq")
    me = lax.axis_index("head")
    stride = seq_count // 8
    z = seq // stride
    far = (1, 2, 4)
    if MODE == "cyclic":
        above = below = [True] * 3
        down_send = up_send = og_sends = back_send_if = back_recv_if = (True, True, True)
    else:
        above = [z + steps <= 7 for steps in far]
        below = [z >= steps for steps in far]
        middle = (z >= 2) & (z <= 5)
        down_send = (z >= 1, (z >= 1) & (z <= 6), middle)
        up_send = (z <= 6, (z >= 1) & (z <= 6), (z == 2) | (z == 4) | (z == 5) if KV_WRAP else middle)
        og_sends = (z >= 1, (z >= 1) & (z <= 6), (z == 2) | (z == 5) if OG_WRAP else middle)
        back_send_if = (z <= 3, z <= 5, z <= 6)
        back_recv_if = (middle, (z >= 1) & (z <= 6), z >= 1)
    og_forward = (z == 7) | (z == 0) if OG_WRAP else False
    og_leaves = (z == 5) | (z == 6) if OG_WRAP else False
    kv_leaves = z == 1 if KV_WRAP else False
    kv_forward = z == 7 if KV_WRAP else False
    mates = (me, me + 1 - 2 * (me % 2), me + 2 - 4 * (me // 2), 3 - me)

    def along(steps):
        return {"seq": lax.rem(seq + (steps % 8) * stride, seq_count)}

    def cols(h):
        if isinstance(h, int):
            return pl.ds(h * HDIM, HDIM)
        return pl.ds(pl.multiple_of(h * HDIM, HDIM), HDIM)

    def remote(source, target, send, recv, device):
        return pltpu.make_async_remote_copy(
            src_ref=source, dst_ref=target, send_sem=send, recv_sem=recv,
            device_id=device, device_id_type=MESH,
        )

    bulk = {"k": (ka, 0, 1), "v": (va, 1, 1), "q": (qa, 2, -1)}

    def move(kind, hop, h):
        ref, row, sign = bulk[kind]
        return remote(
            ref.at[hop, :, cols(h)], ref.at[hop + 1, :, cols(h)],
            bulk_send.at[row, hop, h], bulk_recv.at[row, hop, h],
            along(sign * (2 if hop == 2 else 1)),
        )

    def half_of(half):
        return pl.ds(half * (width // PARTS), width // PARTS)

    def og_move(hop, half):
        part = half_of(half)
        return remote(
            og.at[hop, 0, :, part], og.at[hop + 1, 0, :, part],
            og_send.at[hop, half], og_recv.at[hop, half], along(-(2 if hop == 2 else 1)),
        )

    def og_out(half):
        part = half_of(half)
        return remote(
            og.at[0, 0, :, part], og_wrap.at[:, part],
            hop_send.at[half], hop_recv.at[half], along(2),
        )

    def og_on(half):
        part = half_of(half)
        return remote(
            og_wrap.at[:, part], og.at[3, 0, :, part],
            og_send.at[2, half], og_recv.at[2, half], along(2),
        )

    def kv_out(index, h):
        ref = (ka, va)[index]
        return remote(
            ref.at[0, :, cols(h)], kv_wrap.at[index, :, cols(h - moved)],
            wrap_send.at[index, h], wrap_recv.at[index, h], along(-2),
        )

    def kv_on(index, h):
        ref = (ka, va)[index]
        return remote(
            kv_wrap.at[index, :, cols(h - moved)], ref.at[3, :, cols(h)],
            bulk_send.at[index, 2, h], bulk_recv.at[index, 2, h], along(-2),
        )

    def sends(kind, hop):
        return (down_send if kind == "q" else up_send)[hop]

    def comes(kind, hop):
        return (above if kind == "q" else below)[hop]

    def started(condition, copy):
        @given(condition)
        def _():
            copy().start()

    def landed(condition, copy):
        @given(condition)
        def _():
            copy().wait_recv()

    def left(condition, copy):
        @given(condition)
        def _():
            copy().wait_send()

    def near(slot, which, half):
        source, target, mate = ((0, 1, 1), (0, 2, 2), (2, 3, 1))[which]
        part = half_of(half)
        return remote(
            og.at[slot, source, :, part], og.at[slot, target, :, part],
            near_send.at[slot, which, half], near_recv.at[slot, which, half],
            {"head": mates[mate]},
        )

    def spread(slot, half):
        near(slot, 1, half).start()
        near(slot, 0, half).start()

    def stat_move(hop, h):
        return remote(
            stat_out.at[hop, h], stat_in.at[hop, h], stat_send.at[hop, h], stat_recv.at[hop, h],
            along((1, 2, 4)[hop]),
        )

    def row_move(hop, h):
        return remote(
            row_out.at[hop, h], row_in.at[hop, h], row_send.at[hop, h], row_recv.at[hop, h],
            along(-(1, 2, 4)[hop]),
        )

    def back_move(hop, h):
        return remote(
            back_out.at[hop, :, cols(h)], back_in.at[hop, :, cols(h)],
            back_send.at[hop, h], back_recv.at[hop, h], along((2, 1, 1)[hop]),
        )

    def hidden(hop, h):
        index = SECTIONS - 1 - hop
        inside = (seq >= seq_count // 2 ** (index + 1)).astype(jnp.int32)
        usable = table[index, h] * active[0, index] * inside
        return (1.0 - usable.astype(jnp.float32)) * HIDE

    def causal(raw):
        key_index = lax.broadcasted_iota(jnp.int32, (BLK, BLK), 0)
        query_index = lax.broadcasted_iota(jnp.int32, (BLK, BLK), 1)
        return jnp.where(key_index <= query_index, raw, HIDE)

    def slot_used(slot):
        return True if slot == 0 else above[slot - 1]

    def make_grad(slot):
        @given(slot_used(slot))
        def _():
            for half in range(PARTS):
                near(slot, 0, half).wait_recv()
                near(slot, 2, half).wait_recv()

            @pl.loop(0, heads // 2)
            def _(pair):
                wide = pl.ds(pl.multiple_of(pair * 2 * HDIM, 2 * HDIM), 2 * HDIM)
                total = jnp.zeros((BLK, 2 * HDIM), jnp.float32)
                for index, owner in enumerate(mates):
                    features = pl.ds(pl.multiple_of(owner * width, width), width)
                    total = total + mm(og[slot, index], w[wide, features], NT)
                ga[slot, :, wide] = total.astype(jnp.bfloat16)

    def pass_near(slot):
        @given(slot_used(slot))
        def _():
            for half in range(PARTS):
                near(slot, 1, half).wait_recv()
                near(slot, 2, half).start()

    def pass_og(hop, half):
        @given(above[hop])
        def _():
            og_move(hop, half).wait_recv()
        if hop < 2:
            started(og_sends[hop + 1], lambda: og_move(hop + 1, half))
        @given(above[hop])
        def _():
            spread(hop + 1, half)

    def forward_og(half):
        @given(og_forward)
        def _():
            og_out(half).wait_recv()
            og_on(half).start()

    def forward_kv(h):
        @given(kv_forward)
        def _():
            for index in range(2):
                kv_out(index, h).wait_recv()
                kv_on(index, h).start()

    def query_side(h):
        at = cols(h)
        query = qa[0, :, at]
        grad = ga[0, :, at]
        top = None
        for s in range(SECTIONS + 1):
            raw = mm(ka[s, :, at], query, NT) * SCALE
            raw = causal(raw) if s == 0 else raw + hidden(s - 1, h)
            scores[s] = raw
            high = jnp.max(raw, axis=0, keepdims=True)
            top = high if top is None else jnp.maximum(top, high)
        total = None
        for s in range(SECTIONS + 1):
            part = jnp.exp(scores[s] - top)
            scores[s] = part
            part = jnp.sum(part, axis=0, keepdims=True)
            total = part if total is None else total + part
        inverse = 1.0 / total
        delta = None
        for s in range(SECTIONS + 1):
            probs = scores[s] * inverse
            scores[s] = probs
            weights = probs.astype(jnp.bfloat16)
            slope = mm(va[s, :, at], grad, NT)
            slopes[s] = slope
            part = jnp.sum(weights.astype(jnp.float32) * slope, axis=0, keepdims=True)
            delta = part if delta is None else delta + part
            if s == 0:
                own_dv[:, at] = mm(weights, grad, NN)
        log_norm = top + jnp.log(total)
        for hop in range(SECTIONS):
            row_out[hop, h, 0:1, :] = log_norm - hidden(hop, h)
            row_out[hop, h, 1:2, :] = delta
        query_sum = None
        for s in range(SECTIONS + 1):
            dlogit = (scores[s] * (slopes[s] - delta) * SCALE).astype(jnp.bfloat16)
            part = mm(dlogit, ka[s, :, at], TN)
            query_sum = part if query_sum is None else query_sum + part
            if s == 0:
                own_dk[:, at] = mm(dlogit, query, NN)
        dq[:, at] = query_sum.astype(jnp.bfloat16)
        for hop in range(SECTIONS):
            started(below[hop], lambda hop=hop: row_move(hop, h))

    def key_side(h):
        at = cols(h)
        key = ka[0, :, at]
        value = va[0, :, at]
        key_sum = own_dk[:, at]
        value_sum = own_dv[:, at]
        for hop in range(SECTIONS):
            query = qa[hop + 1, :, at]
            grad = ga[hop + 1, :, at]
            log_norm = row_in[hop, h, 0:1, :]
            delta = row_in[hop, h, 1:2, :]
            probs = jnp.exp(mm(key, query, NT) * SCALE - log_norm)
            slope = mm(value, grad, NT)
            dlogit = (probs * (slope - delta) * SCALE).astype(jnp.bfloat16)
            key_sum = key_sum + mm(dlogit, query, NN)
            value_sum = value_sum + mm(probs.astype(jnp.bfloat16), grad, NN)
        dk[:, at] = key_sum.astype(jnp.bfloat16)
        dv[:, at] = value_sum.astype(jnp.bfloat16)

    def partial_scores(slot, h):
        at = cols(h)
        raw = mm(ka[0, :, at], qa[slot, :, at], NT) * SCALE
        if slot == 0:
            raw = causal(raw)
        top = jnp.max(raw, axis=0, keepdims=True)
        part = jnp.exp(raw - top)
        slope = mm(va[0, :, at], ga[slot, :, at], NT)
        held_p[slot, h] = part
        held_s[slot, h] = slope
        total = jnp.sum(part, axis=0, keepdims=True)
        drift = jnp.sum(part * slope, axis=0, keepdims=True)
        tops[slot, h, 0:1, :] = top
        return top, total, drift

    def stage_own(h):
        top, total, drift = partial_scores(0, h)
        norms[h, 0:1, :] = total
        norms[h, 1:2, :] = drift

    def stage_a(h):
        landed(comes("q", 2), lambda: move("q", 2, h))
        for hop in range(SECTIONS):
            top, total, drift = partial_scores(hop + 1, h)
            stat_out[hop, h, 0:1, :] = top
            stat_out[hop, h, 1:2, :] = total
            stat_out[hop, h, 2:3, :] = drift
            stat_out[hop, h, 3:4, :] = drift
            started(above[hop], lambda hop=hop: stat_move(hop, h))

    def stage_b(h):
        for hop in range(SECTIONS):
            landed(below[hop], lambda hop=hop: stat_move(hop, h))
        tops_of = [tops[0, h, 0:1, :]] + [
            stat_in[hop, h, 0:1, :] + hidden(hop, h) for hop in range(SECTIONS)
        ]
        top = functools.reduce(jnp.maximum, tops_of)
        factor = jnp.exp(tops_of[0] - top)
        total = factor * norms[h, 0:1, :]
        drift = factor * norms[h, 1:2, :]
        for hop in range(SECTIONS):
            factor = jnp.exp(tops_of[hop + 1] - top)
            total = total + factor * stat_in[hop, h, 1:2, :]
            drift = drift + factor * stat_in[hop, h, 2:3, :]
        log_norm = top + jnp.log(total)
        delta = drift / total
        norms[h, 0:1, :] = log_norm
        norms[h, 1:2, :] = delta
        for hop in range(SECTIONS):
            row_out[hop, h, 0:1, :] = log_norm - hidden(hop, h)
            row_out[hop, h, 1:2, :] = delta
            started(below[hop], lambda hop=hop: row_move(hop, h))

    def stage_c(h):
        at = cols(h)
        for hop in range(SECTIONS):
            landed(above[hop], lambda hop=hop: row_move(hop, h))
        key_sum = None
        value_sum = None
        for slot in (3, 2, 1, 0):
            if slot == 0:
                log_norm, delta = norms[h, 0:1, :], norms[h, 1:2, :]
            else:
                log_norm, delta = row_in[slot - 1, h, 0:1, :], row_in[slot - 1, h, 1:2, :]
            probs = held_p[slot, h] * jnp.exp(tops[slot, h, 0:1, :] - log_norm)
            dlogit = (probs * (held_s[slot, h] - delta) * SCALE).astype(jnp.bfloat16)
            query_part = mm(dlogit, ka[0, :, at], TN)
            if slot == 3:
                back_out[0, :, at] = query_part.astype(jnp.bfloat16)
            else:
                parts[slot, :, at] = query_part
            key_part = mm(dlogit, qa[slot, :, at], NN)
            value_part = mm(probs.astype(jnp.bfloat16), ga[slot, :, at], NN)
            key_sum = key_part if key_sum is None else key_sum + key_part
            value_sum = value_part if value_sum is None else value_sum + value_part
        dk[:, at] = key_sum.astype(jnp.bfloat16)
        dv[:, at] = value_sum.astype(jnp.bfloat16)
        started(back_send_if[0], lambda: back_move(0, h))

    def stage_back(hop, h):
        at = cols(h)
        landed(back_recv_if[hop], lambda: back_move(hop, h))
        total = (parts[2 - hop, :, at] + back_in[hop, :, at].astype(jnp.float32)).astype(jnp.bfloat16)
        if hop == 2:
            dq[:, at] = total
        else:
            back_out[hop + 1, :, at] = total
            started(back_send_if[hop + 1], lambda: back_move(hop + 1, h))

    copies = [
        pltpu.make_async_copy(source, target, local_sem.at[index])
        for index, (source, target) in enumerate(
            ((og_in, og.at[0, 0]), (q_in, qa.at[0]), (k_in, ka.at[0]), (v_in, va.at[0]), (w_in, w))
        )
    ]
    for copy in copies:
        copy.start()

    def fill(ref, value=0.0):
        ref[...] = jnp.full(ref.shape, value, ref.dtype)

    for slot in range(1, SECTIONS + 1):
        @given(opposite(above[slot - 1]))
        def _(slot=slot):
            fill(qa.at[slot])
            fill(ga.at[slot])
            fill(row_in.at[slot - 1], -HIDE)

        @given(opposite(below[slot - 1]))
        def _(slot=slot):
            fill(ka.at[slot])
            fill(va.at[slot])
            fill(stat_in.at[slot - 1])

        @given(opposite(back_recv_if[slot - 1]))
        def _(slot=slot):
            fill(back_in.at[slot - 1])

    barrier = pltpu.get_barrier_semaphore()
    for steps in (1, -1, 2, -2, 4):
        pl.semaphore_signal(barrier, inc=1, device_id=along(steps), device_id_type=MESH)
    for mate in mates[1:3]:
        pl.semaphore_signal(barrier, inc=1, device_id={"head": mate}, device_id_type=MESH)
    pl.semaphore_wait(barrier, 7)

    def each(first, last):
        return pl.loop(first, last)

    def begin(kinds, hop, first, last, condition=None):
        @given(sends(kinds[0], hop) if condition is None else condition)
        def _():
            @each(first, last)
            def _(h):
                for kind in kinds:
                    move(kind, hop, h).start()

    def relay(kind, hop, h):
        landed(comes(kind, hop), lambda: move(kind, hop, h))
        started(sends(kind, hop + 1), lambda: move(kind, hop + 1, h))

    def late_query_side(h):
        for kind in "kv":
            landed(comes(kind, 2), lambda kind=kind: move(kind, 2, h))
        query_side(h)

    def late_key_side(h):
        landed(comes("q", 2), lambda: move("q", 2, h))
        for hop in range(SECTIONS):
            landed(above[hop], lambda hop=hop: row_move(hop, h))
        key_side(h)

    def relay_kv(hop, h):
        relay("k", hop, h)
        relay("v", hop, h)

    def send_kv_round(first, last):
        @given(kv_leaves)
        def _():
            @each(first, last)
            def _(h):
                kv_out(0, h).start()
                kv_out(1, h).start()

    copies[0].wait()
    for half in range(PARTS):
        started(og_sends[0], lambda half=half: og_move(0, half))
    for half in range(PARTS):
        spread(0, half)
    for half in range(PARTS):
        started(og_leaves, lambda half=half: og_out(half))
    copies[2].wait()
    copies[3].wait()
    begin("kv", 0, moved, heads)
    copies[1].wait()
    pass_og(0, 0)
    pass_og(0, 1)
    pass_og(0, 2)
    pass_og(0, 3)
    begin("q", 0, 0, 4)
    begin("q", 0, 4, 8, z >= EARLY)
    pass_og(1, 0)
    forward_og(0)
    pass_og(1, 1)
    forward_og(1)
    relay_kv(0, 4)
    pass_og(1, 2)
    forward_og(2)
    pass_og(1, 3)
    forward_og(3)
    relay_kv(0, 5)
    pass_near(0)
    copies[4].wait()
    make_grad(0)
    relay_kv(0, 6)
    relay_kv(0, 7)
    pass_near(1)
    relay("q", 0, 0)
    relay("q", 0, 1)
    relay("q", 0, 2)
    relay("q", 0, 3)
    send_kv_round(4, 6)
    make_grad(1)
    pass_og(2, 0)
    pass_og(2, 1)
    stage_own(0)
    stage_own(1)
    stage_own(2)
    stage_own(3)
    pass_og(2, 2)
    pass_og(2, 3)
    relay("q", 1, 0)
    pass_near(2)
    make_grad(2)
    relay("q", 1, 1)
    relay("q", 1, 2)
    pass_near(3)
    make_grad(3)
    stage_a(0)
    relay_kv(1, 4)
    stage_a(1)
    relay("q", 1, 3)
    begin("q", 0, 4, 6, (z >= 1) & (z < EARLY))
    relay_kv(1, 5)
    forward_kv(4)
    stage_b(0)
    begin("q", 0, 6, 8, (z >= 1) & (z < EARLY))
    forward_kv(5)
    stage_a(2)
    relay_kv(1, 6)
    stage_b(1)
    relay("q", 0, 4)
    stage_a(3)
    relay("q", 0, 5)
    send_kv_round(6, 8)
    relay_kv(1, 7)
    late_query_side(4)
    stage_b(2)
    relay("q", 0, 6)
    stage_c(0)
    late_query_side(5)
    stage_b(3)
    relay("q", 0, 7)
    stage_c(1)
    forward_kv(6)
    relay("q", 1, 4)
    stage_back(0, 0)
    relay("q", 1, 5)
    stage_c(2)
    forward_kv(7)
    relay("q", 1, 6)
    late_query_side(6)
    stage_c(3)
    relay("q", 1, 7)
    late_query_side(7)
    stage_back(0, 1)
    stage_back(1, 0)
    stage_back(0, 2)
    stage_back(1, 1)
    stage_back(0, 3)
    stage_back(2, 0)
    stage_back(1, 2)
    late_key_side(4)
    stage_back(2, 1)
    stage_back(1, 3)
    late_key_side(5)
    stage_back(2, 2)
    late_key_side(6)
    stage_back(2, 3)
    late_key_side(7)

    @each(0, heads)
    def _(h):
        for hop in range(SECTIONS):
            left(below[hop], lambda hop=hop: row_move(hop, h))
            left(down_send[hop], lambda hop=hop: move("q", hop, h))

    @each(0, moved)
    def _(h):
        for hop in range(SECTIONS):
            left(above[hop], lambda hop=hop: stat_move(hop, h))
            left(back_send_if[hop], lambda hop=hop: back_move(hop, h))

    @each(moved, heads)
    def _(h):
        for hop in range(SECTIONS):
            for kind in "kv":
                left(up_send[hop], lambda kind=kind, hop=hop: move(kind, hop, h))
        for index in range(2):
            left(kv_leaves, lambda index=index: kv_out(index, h))
            left(kv_forward, lambda index=index: kv_on(index, h))

    for half in range(PARTS):
        left(og_leaves, lambda half=half: og_out(half))
        left(og_forward, lambda half=half: og_on(half))
        for hop in range(SECTIONS):
            left(og_sends[hop], lambda hop=hop, half=half: og_move(hop, half))
        for slot in range(SECTIONS + 1):
            for which in range(3):
                left(slot_used(slot), lambda slot=slot, which=which, half=half: near(slot, which, half))


def write_out(dq, dk, dv, dq_out, dk_out, dv_out, sem):
    copies = [
        pltpu.make_async_copy(source, target, sem.at[index])
        for index, (source, target) in enumerate(((dq, dq_out), (dk, dk_out), (dv, dv_out)))
    ]
    for copy in copies:
        copy.start()
    for copy in copies:
        copy.wait()


def body(queries, key_rows, value_rows, out_grad, out_proj, section_table, block_active):
    seq_count = lax.axis_size("seq")
    heads = queries.shape[1] // HDIM
    moved = heads // 2
    width = queries.shape[1]
    part = moved * HDIM
    four = (SECTIONS + 1, BLK, width)
    any_space = pl.BlockSpec(memory_space=pl.ANY)
    vmem = pl.BlockSpec(memory_space=pltpu.VMEM)
    smem = pl.BlockSpec(memory_space=pltpu.SMEM)
    out = jax.ShapeDtypeStruct((BLK, width), jnp.bfloat16)
    bf16, f32, dma = jnp.bfloat16, jnp.float32, pltpu.SemaphoreType.DMA
    placed = [
        pltpu.with_memory_space_constraint(array, pltpu.HBM)
        for array in (
            section_table.T, block_active, queries, key_rows, value_rows, out_grad, out_proj
        )
    ]
    grads = pl.pallas_call(
        functools.partial(kernel, seq_count, moved),
        out_shape=(out, out, out),
        in_specs=[smem, smem] + [pl.BlockSpec(memory_space=pltpu.HBM)] * 5,
        out_specs=(vmem, vmem, vmem),
        scratch_shapes=[
            pltpu.VMEM(four, bf16),
            pltpu.VMEM(four, bf16),
            pltpu.VMEM(four, bf16),
            pltpu.VMEM(four, bf16),
            pltpu.VMEM((SECTIONS + 1, 4, *out_grad.shape), bf16),
            pltpu.VMEM(out_grad.shape, bf16),
            pltpu.VMEM((2, BLK, width - part), bf16),
            pltpu.VMEM(out_proj.shape, bf16),
            pltpu.VMEM((SECTIONS + 1, BLK, BLK), f32),
            pltpu.VMEM((SECTIONS + 1, BLK, BLK), f32),
            pltpu.VMEM((SECTIONS + 1, moved, BLK, BLK), f32),
            pltpu.VMEM((SECTIONS + 1, moved, BLK, BLK), f32),
            pltpu.VMEM((SECTIONS + 1, moved, 8, BLK), f32),
            pltpu.VMEM((moved, 8, BLK), f32),
            pltpu.VMEM((BLK, width), f32),
            pltpu.VMEM((BLK, width), f32),
            pltpu.VMEM((SECTIONS, BLK, part), f32),
            pltpu.VMEM((SECTIONS, moved, 4, BLK), f32),
            pltpu.VMEM((SECTIONS, moved, 4, BLK), f32),
            pltpu.VMEM((SECTIONS, heads, 2, BLK), f32),
            pltpu.VMEM((SECTIONS, heads, 2, BLK), f32),
            pltpu.VMEM((SECTIONS, BLK, part), bf16),
            pltpu.VMEM((SECTIONS, BLK, part), bf16),
            dma((5,)),
            dma((SECTIONS, PARTS)),
            dma((SECTIONS, PARTS)),
            dma((PARTS,)),
            dma((PARTS,)),
            dma((2, heads)),
            dma((2, heads)),
            dma((SECTIONS + 1, 3, PARTS)),
            dma((SECTIONS + 1, 3, PARTS)),
            dma((3, SECTIONS, heads)),
            dma((3, SECTIONS, heads)),
            dma((SECTIONS, moved)),
            dma((SECTIONS, moved)),
            dma((SECTIONS, heads)),
            dma((SECTIONS, heads)),
            dma((SECTIONS, moved)),
            dma((SECTIONS, moved)),
        ],
        compiler_params=pltpu.CompilerParams(
            collective_id=0, has_side_effects=True, vmem_limit_bytes=44 * 1024 * 1024
        ),
        name="attention_grads",
    )(*placed)
    return pl.pallas_call(
        write_out,
        out_shape=(out, out, out),
        in_specs=[vmem] * 3,
        out_specs=[any_space] * 3,
        scratch_shapes=[dma((3,))],
        compiler_params=pltpu.CompilerParams(vmem_limit_bytes=4 * 1024 * 1024),
        name="write_out",
    )(*grads)


def solution(mesh):
    return jax.shard_map(
        body,
        mesh=mesh,
        in_specs=(
            P("seq", "head"),
            P("seq", "head"),
            P("seq", "head"),
            P("seq", "head"),
            P("head", None),
            P("head", None),
            P("seq", None),
        ),
        out_specs=(P("seq", "head"), P("seq", "head"), P("seq", "head")),
        check_vma=False,
    )
```
